128 devices in a mesh: dom: 32 (over x, y, core), shift: 4 (over z).
Axes of the slice: x: 4, y: 4, z: 4, core: 2. Of those that a mesh axis runs over, the one named last changes fastest.
Arguments:
- sources: float32 [32, 128, 16, 128], P('shift', 'dom'), may hold values from -6 to 6
- kappa: float32 [128, 16, 128], P('dom'), may hold values from 0 to 2
- mass: float32 [128, 16, 128], P('dom'), may hold values from 0.25 to 4
- shift_table: float32 [64], replicated, may hold values from 0.5 to 4
- shift_ids: int32 [16], P('shift'), may hold values from 0 to 63
- sketch: bfloat16 [1024, 128, 16, 128], P(None, 'dom'), may hold values from -0.1875 to 0.1875
Outputs:
- solution: float32 [16, 32, 128, 16, 128], P('shift', None, 'dom')
- residual: float32 [16, 32, 128, 16, 128], P('shift', None, 'dom')
The draws below stay inside these ranges and needn't reach their ends.
Inputs may be any that keep to these rules, and one draw needn't show every extreme that they name: `shift_ids`: index into shift_table.
All inputs are finite; a program needn't handle non-finite values.
Results may differ from the reference program's by a relative error of at most 0.0026.
Values sent between devices are 32-bit elements; how exact they have to be, the bound alone decides.
No kernel may reach another device: no remote copies, remote signals or barrier semaphores. Data moves between devices by JAX's collectives and lax.ppermute only.
A program may use at most 128 MiB of HBM per device.

```python
import math
import jax
import jax.numpy as jnp
from jax import lax

SK = 1024
SHIFTS = 16
TABLE = 64
NY = 16
NZ = 128
B = 32
NX = 128


def plant(array, stream_key, least, top_value):
    dims = array.shape
    place = [jax.random.randint(jax.random.fold_in(stream_key, axis), (), 0, dims[axis]) for axis in range(len(dims))]
    array = array.at[tuple(place)].set(least)
    longest = dims.index(max(dims))
    place[longest] = (place[longest] + 1) % dims[longest]
    return array.at[tuple(place)].set(top_value)


def block_scale(own_key, shape, cuts, least, largest):
    gain, own = 1.0, jax.random.fold_in(own_key, 6)
    for dim, blocks in cuts:
        steps = jnp.exp(jax.random.uniform(jax.random.fold_in(own, dim), (blocks,), jnp.float32, least / len(cuts), largest / len(cuts)))
        gain = gain * jnp.repeat(steps, shape[dim] // blocks).reshape([-1 if axis == dim else 1 for axis in range(len(shape))])
    return gain


def gaussian(key, shape, deviation, reach, pieces=(), held_as=jnp.bfloat16):
    drawn = jax.random.normal(key, shape, jnp.float32) * deviation
    if len(pieces) > 0:
        drawn = block_scale(key, shape, pieces, -0.22, 0.18) * drawn
    return jnp.clip(drawn, min=-reach, max=reach).astype(held_as)


def setup_inputs(seed: int = 0) -> dict:
    splits = jax.random.split(jax.random.key(seed), 7)
    return {
        "sources": gaussian(splits[0], (B, NX, NY, NZ), 1.0, 6.0, ((0, 4), (1, 32)), jnp.float32),
        "kappa": jnp.clip(2.0 * jax.random.uniform(splits[1], (NX, NY, NZ), jnp.float32) ** block_scale(splits[1], (NX, NY, NZ), ((0, 32),), -0.2, 0.2), 0.0, 2.0),
        "mass": jnp.clip(jnp.exp(math.log(4.0) - 2.7725887 * jax.random.uniform(splits[2], (NX, NY, NZ), jnp.float32) ** block_scale(splits[2], (NX, NY, NZ), ((0, 32),), -0.2, 0.2)), 0.25, 4.0),
        "shift_table": jnp.clip(jax.random.uniform(splits[3], (TABLE,), jnp.float32, 0.5, 4.0), 0.5, 4.0),
        "shift_ids": plant(jax.random.randint(splits[4], (SHIFTS,), 0, TABLE), jax.random.fold_in(splits[4], 1), 0, TABLE - 1).astype(jnp.int32),
        "sketch": gaussian(splits[5], (SK, NX, NY, NZ), SK ** -0.5, 0.1875, ((1, 32),)),
    }


def shift_values(shift_table, shift_ids):
    entries = jnp.arange(shift_table.shape[0], dtype=jnp.int32)
    picked = jnp.where(shift_ids[:, None] == entries[None, :], shift_table[None, :], 0.0)
    return lax.optimization_barrier(jnp.sum(picked, axis=1))

def apply_operator(field, diag):
    padded = jnp.pad(field, ((0, 0), (1, 1), (1, 1), (1, 1)))
    beside = padded[:, 2:, 1:-1, 1:-1] + padded[:, :-2, 1:-1, 1:-1]
    beside = beside + padded[:, 1:-1, 2:, 1:-1] + padded[:, 1:-1, :-2, 1:-1]
    beside = beside + padded[:, 1:-1, 1:-1, 2:] + padded[:, 1:-1, 1:-1, :-2]
    return diag * field - beside

def solve_small(gram):
    h_vals = [gram[:, 1 + i, 0] for i in range(3)]
    ridge = 0.001 * (gram[:, 1, 1] + gram[:, 2, 2] + gram[:, 3, 3]) / 3.0 + 1.0
    entry = [[gram[:, 1 + i, 1 + k] + (ridge if i == k else 0.0) for k in range(3)] for i in range(3)]
    l00 = jnp.sqrt(entry[0][0])
    l10 = entry[1][0] / l00
    l20 = entry[2][0] / l00
    l11 = jnp.sqrt(entry[1][1] - l10 * l10)
    l21 = (entry[2][1] - l20 * l10) / l11
    l22 = jnp.sqrt(entry[2][2] - l20 * l20 - l21 * l21)
    f0 = h_vals[0] / l00
    f1 = (h_vals[1] - l10 * f0) / l11
    f2 = (h_vals[2] - l20 * f0 - l21 * f1) / l22
    c2 = f2 / l22
    c1 = (f1 - l21 * c2) / l11
    c0 = (f0 - l10 * c1 - l20 * c2) / l00
    return (c0, c1, c2)

def gram_of(sketched):
    return jnp.einsum('rib,rkb->bik', sketched, sketched, precision=lax.Precision.HIGHEST)

def reference(sources, kappa, mass, shift_table, shift_ids, sketch):
    sigma = shift_values(shift_table, shift_ids)
    matrix = sketch.reshape(sketch.shape[0], -1)
    count = sources.shape[0]

    def one_shift(value):
        diag = (6.0 - kappa + value * mass)[None]
        center = 6.0 + value
        w0 = sources
        z0 = apply_operator(w0, diag)
        w1 = (z0 - center * w0) / 6.0
        z1 = apply_operator(w1, diag)
        w2 = (z1 - center * w1) / 6.0
        z2 = apply_operator(w2, diag)
        stacked = jnp.stack([w0, z0, z1, z2], axis=0).astype(jnp.bfloat16).reshape(4 * count, -1)
        sketched = lax.dot_general(matrix, stacked, (((1,), (1,)), ((), ())), preferred_element_type=jnp.float32)
        gram = gram_of(sketched.reshape(matrix.shape[0], 4, count))
        c0, c1, c2 = solve_small(gram)
        c0 = c0[:, None, None, None]
        c1 = c1[:, None, None, None]
        c2 = c2[:, None, None, None]
        solution = c0 * w0 + c1 * w1 + c2 * w2
        residual = w0 - c0 * z0 - c1 * z1 - c2 * z2
        return (solution, residual)
    solution, residual = lax.map(one_shift, sigma)
    return (solution, residual)
```

```python
import functools

import jax
import jax.numpy as jnp
from jax import lax
from jax.experimental import pallas as pl
from jax.experimental.pallas import tpu as pltpu
from jax.sharding import PartitionSpec as P


BOTH = ("dom", "shift")
FIELDS = 10
LEVEL = (0, 1, 1, 2, 2, 2, 3, 3, 3, 3)
POWER = (0, 0, 1, 0, 1, 2, 0, 1, 2, 3)
SIGN = (1.0, -1.0, 1.0, 1.0, -1.0, 1.0, -1.0, 1.0, -1.0, 1.0)
PITCH = 12
VMEM = pl.BlockSpec(memory_space=pltpu.VMEM)
SMEM = pl.BlockSpec(memory_space=pltpu.SMEM)


def around(field):
    inner = field[1:-1]
    rows = lax.broadcasted_iota(jnp.int32, inner.shape, 1)
    lanes = lax.broadcasted_iota(jnp.int32, inner.shape, 2)
    ny, nz = inner.shape[1], inner.shape[2]
    total = field[2:] + field[:-2]
    total = total + jnp.where(rows == 0, 0.0, pltpu.roll(inner, 1, 1))
    total = total + jnp.where(rows == ny - 1, 0.0, pltpu.roll(inner, ny - 1, 1))
    total = total + jnp.where(lanes == 0, 0.0, pltpu.roll(inner, 1, 2))
    return total + jnp.where(lanes == nz - 1, 0.0, pltpu.roll(inner, nz - 1, 2))


def masked(field, count, low, high):
    return jnp.concatenate([field[:count] * low, field[count:-count], field[-count:] * high], axis=0)


def ten_fields(w, kappa, q, low, high):
    def p(field, planes):
        cut = (kappa.shape[0] - planes) // 2
        return kappa[cut : cut + planes] * field[1:-1] + around(field)

    slab = w.shape[0] - 6
    e10 = masked(p(w, slab + 4), 2, low, high)
    e01 = q[1:-1] * w[1:-1]
    e20 = masked(p(e10, slab + 2), 1, low, high)
    e11 = masked(p(e01, slab + 2) + q[2:-2] * e10[1:-1], 1, low, high)
    e02 = q[2:-2] * e01[1:-1]
    q3 = q[3:-3]
    e30 = p(e20, slab)
    e21 = p(e11, slab) + q3 * e20[1:-1]
    e12 = p(e02, slab) + q3 * e11[1:-1]
    e03 = q3 * e02[1:-1]
    return (w[3:-3], e10[2:-2], e01[2:-2], e20[1:-1], e11[1:-1], e02[1:-1], e30, e21, e12, e03)


def sketch_kernel(edge, own, low, high, sketch, out, held, fld, right, acc0, acc1, cols0, cols1, sem):
    sources = own.shape[0] - 2
    slab, ny, nz = own.shape[1:]
    blocks, block = sem.shape[0], held.shape[1] // sem.shape[0]
    pairs = held.shape[0]

    def fetch(b, k):
        rows = pl.ds(b * block, block)
        return pltpu.make_async_copy(sketch.at[rows, k], held.at[k, rows], sem.at[b])

    for b in range(blocks):
        for k in range(pairs):
            fetch(b, k).start()

    low_on, high_on = edge[0], edge[1]
    kappa = jnp.concatenate([low[0], own[0], high[0]], axis=0)
    q = jnp.concatenate([low[1], own[1], high[1]], axis=0) - 1.0
    pitch = fld.shape[0] // (FIELDS * sources)

    def one_source(s, carry):
        w = jnp.concatenate([low[s + 2], own[s + 2], high[s + 2]], axis=0)
        for f, field in enumerate(ten_fields(w, kappa, q, low_on, high_on)):
            start = pl.multiple_of((f * sources + s) * pitch, 8)
            fld[pl.ds(start, slab * ny), :] = field.reshape(slab * ny, nz)
        return carry

    lax.fori_loop(0, sources, one_source, 0)
    columns = FIELDS * sources
    for k in range(pairs):
        for parity in range(2):
            rows = fld[pl.ds(2 * k + parity, columns, stride=pitch), :]
            right[pl.ds(parity * 128, columns), k * nz : (k + 1) * nz] = rows.astype(jnp.bfloat16)

    half = block // 2
    for b in range(blocks):
        for k in range(pairs):
            fetch(b, k).wait()
        left = jnp.concatenate(
            [held[k, b * block : (b + 1) * block].reshape(2 * block, nz) for k in range(pairs)], axis=1
        )
        both = lax.dot_general(left, right[...], (((1,), (1,)), ((), ())), preferred_element_type=jnp.float32)
        acc0[...] = both[:, :128]
        acc1[...] = both[:, 128:]
        rows = acc0[pl.ds(0, block, stride=2), :] + acc1[pl.ds(1, block, stride=2), :]
        cols0[...] = rows[:half].T
        cols1[...] = rows[half:].T
        for s in range(sources):
            piece = s * blocks + b
            out[piece, 0:FIELDS, :] = cols0[pl.ds(s, FIELDS, stride=sources), :]
            out[piece, FIELDS : 2 * FIELDS, :] = cols1[pl.ds(s, FIELDS, stride=sources), :]
            out[piece, 2 * FIELDS :, :] = jnp.zeros((out.shape[1] - 2 * FIELDS, 128), jnp.float32)


def gram_kernel(pieces, out):
    rows = pieces[0]
    for peer in range(1, pieces.shape[0]):
        rows = rows + pieces[peer]
    gram = lax.dot_general(
        rows, rows, (((1,), (1,)), ((), ())), preferred_element_type=jnp.float32, precision=lax.Precision.HIGHEST
    )
    gram = gram[:FIELDS, :FIELDS] + gram[FIELDS : 2 * FIELDS, FIELDS : 2 * FIELDS]
    wide = jnp.concatenate([gram, jnp.zeros((FIELDS, 128 - FIELDS), jnp.float32)], axis=1)
    line = wide[0:1]
    for f in range(1, FIELDS):
        line = line + pltpu.roll(wide[f : f + 1], PITCH * f, 1)
    out[...] = jnp.broadcast_to(line[None], out.shape)


def powers_kernel(edge, table, ids, coeffs, coeff_low, coeff_high, slabs, halos, out):
    low_on, high_on = edge[0], edge[1]
    kappa = jnp.concatenate([coeff_low[0], coeffs[0], coeff_high[0]], axis=0)
    q = jnp.concatenate([coeff_low[1], coeffs[1], coeff_high[1]], axis=0) - 1.0
    shifts = ids.shape[0]
    sigma = [table[ids[j]] for j in range(shifts)]

    def one_source(s, carry):
        w = jnp.concatenate([halos[s, :3], slabs[s], halos[s, 3:]], axis=0)
        _, e10, e01, e20, e11, e02, e30, e21, e12, e03 = ten_fields(w, kappa, q, low_on, high_on)
        for j in range(shifts):
            x = sigma[j]
            out[s, j, 0] = x * e01 - e10
            out[s, j, 1] = x * (x * e02 - e11) + e20
            out[s, j, 2] = x * (x * (x * e03 - e12) + e21) - e30
        return carry

    lax.fori_loop(0, slabs.shape[0], one_source, 0)


def solve_small(gram):
    ridge = 0.001 * (gram[1][1] + gram[2][2] + gram[3][3]) / 3.0 + 1.0
    entry = [[gram[1 + i][1 + k] + (ridge if i == k else 0.0) for k in range(3)] for i in range(3)]
    h = [gram[1 + i][0] for i in range(3)]
    l00 = jnp.sqrt(entry[0][0])
    l10 = entry[1][0] / l00
    l20 = entry[2][0] / l00
    l11 = jnp.sqrt(entry[1][1] - l10 * l10)
    l21 = (entry[2][1] - l20 * l10) / l11
    l22 = jnp.sqrt(entry[2][2] - l20 * l20 - l21 * l21)
    f0 = h[0] / l00
    f1 = (h[1] - l10 * f0) / l11
    f2 = (h[2] - l20 * f0 - l21 * f1) / l22
    c2 = f2 / l22
    c1 = (f1 - l21 * c2) / l11
    c0 = (f0 - l10 * c1 - l20 * c2) / l00
    return c0, c1, c2


def final_kernel(table, ids, grams, w0, powers, sol, res, weights, scalars, sem):
    groups, per_group = 4, w0.shape[0] // 4
    shifts = ids.shape[0]
    step = pl.program_id(0)

    @pl.when(step == 0)
    def _():
        parts = grams.shape[0] // (groups * per_group)
        flat = grams.reshape(grams.shape[0], 128)
        lines = []
        for g in range(groups):
            line = None
            for part in range(parts):
                one = flat[pl.ds(part * groups + g, per_group, stride=parts * groups), :]
                line = one if line is None else line + one
            lines.append(line)
        gram = jnp.concatenate(lines, axis=0)
        lane = lax.broadcasted_iota(jnp.int32, gram.shape, 1)
        sigma = jnp.zeros(gram.shape, jnp.float32)
        for j in range(shifts):
            sigma = jnp.where(lane == j, table[ids[j]], sigma)
        terms = {}
        for f in range(FIELDS):
            for e in range(f, FIELDS):
                place = PITCH * f + e
                value = jnp.broadcast_to(gram[:, place : place + 1], gram.shape)
                sign = SIGN[f] * SIGN[e] * (2.0 if LEVEL[f] == LEVEL[e] and f != e else 1.0)
                value = value if sign == 1.0 else value * sign
                key = (LEVEL[f], LEVEL[e], POWER[f] + POWER[e])
                terms[key] = terms[key] + value if key in terms else value
        inner = [[None] * 4 for _ in range(4)]
        for a in range(4):
            for b in range(a, 4):
                value = terms[(a, b, a + b)]
                for power in range(a + b - 1, -1, -1):
                    value = value * sigma + terms[(a, b, power)]
                value = value * (1.0 / 6.0 ** (a + b))
                inner[a][b] = inner[b][a] = value
        center = 6.0 + sigma
        mixed = [[6.0 * inner[i + 1][k] + center * inner[i][k] for k in range(4)] for i in range(3)]
        full = [[None] * 4 for _ in range(4)]
        for i in range(3):
            full[1 + i][0] = mixed[i][0]
            for k in range(3):
                full[1 + i][1 + k] = 6.0 * mixed[i][k + 1] + center * mixed[i][k]
        c0, c1, c2 = solve_small(full)
        rows = gram.shape[0]
        values = (
            c0,
            c1 * (1.0 / 6.0),
            c2 * (1.0 / 36.0),
            1.0 - c0 * center,
            (6.0 * c0 + c1 * center) * (-1.0 / 6.0),
            (6.0 * c1 + c2 * center) * (-1.0 / 36.0),
            c2 * (-1.0 / 36.0),
        )
        for n, value in enumerate(values):
            weights[n * rows : (n + 1) * rows, :] = value
        copy = pltpu.make_async_copy(weights, scalars, sem)
        copy.start()
        copy.wait()

    here = sol.shape[1]
    rows = w0.shape[0]
    for i in range(here):
        s = step * here + i
        w = w0[s]
        for j in range(shifts):
            v1, v2, v3 = powers[s, j, 0], powers[s, j, 1], powers[s, j, 2]
            c = [scalars[n * rows + s, j] for n in range(7)]
            sol[j, i] = c[0] * w + c[1] * v1 + c[2] * v2
            res[j, i] = c[3] * w + c[4] * v1 + c[5] * v2 + c[6] * v3


def limit(mib):
    return pltpu.CompilerParams(vmem_limit_bytes=mib << 20)


def on_device(sources, kappa, mass, shift_table, shift_ids, sketch):
    f32 = jnp.float32
    dom, shift = lax.axis_size("dom"), lax.axis_size("shift")
    per_group, slab, ny, nz = sources.shape
    total = per_group * shift
    rows = sketch.shape[0]
    pairs = slab * ny // 2
    at = lax.axis_index("dom")
    edge = jnp.stack([at > 0, at < dom - 1]).astype(f32)

    own = jnp.concatenate([kappa[None], mass[None], sources], axis=0)
    forward = [(i, i + 1) for i in range(dom - 1)]
    backward = [(i + 1, i) for i in range(dom - 1)]
    low = lax.ppermute(own[:, slab - 3 :], "dom", forward)
    high = lax.ppermute(own[:, :3], "dom", backward)

    def to_groups(array):
        copies = jnp.broadcast_to(array, (shift, *array.shape))
        return lax.all_to_all(copies, "shift", 0, 0, tiled=True).reshape(total, *array.shape[1:])

    slabs = to_groups(sources)

    blocks = dom // per_group
    block = rows // blocks
    pieces = pl.pallas_call(
        sketch_kernel,
        in_specs=[SMEM, VMEM, VMEM, VMEM, pl.BlockSpec(memory_space=pltpu.HBM)],
        out_specs=VMEM,
        out_shape=jax.ShapeDtypeStruct((dom, 24, 128), f32),
        scratch_shapes=[
            pltpu.VMEM((pairs, rows, 2, nz), jnp.bfloat16),
            pltpu.VMEM((FIELDS * per_group * (slab * ny + 8), nz), f32),
            pltpu.VMEM((256, pairs * nz), jnp.bfloat16),
            pltpu.VMEM((2 * block, 128), f32),
            pltpu.VMEM((2 * block, 128), f32),
            pltpu.VMEM((128, block // 2), f32),
            pltpu.VMEM((128, block // 2), f32),
            pltpu.SemaphoreType.DMA((blocks,)),
        ],
        compiler_params=limit(34),
        name="sketch_fields",
    )(edge, own, low, high, sketch.reshape(rows, pairs, 2, nz))
    halos = to_groups(jnp.concatenate([low[2:], high[2:]], axis=1))
    arrived = lax.all_to_all(pieces, "dom", 0, 0, tiled=True)
    lines = pl.pallas_call(
        gram_kernel,
        in_specs=[VMEM],
        out_specs=VMEM,
        out_shape=jax.ShapeDtypeStruct((dom * shift, 1, 128), f32),
        name="gram",
    )(arrived)
    grams = lax.all_to_all(lines, BOTH, 0, 0, tiled=True)

    shifts = shift_ids.shape[0]
    powers = pl.pallas_call(
        powers_kernel,
        in_specs=[SMEM, SMEM, SMEM, VMEM, VMEM, VMEM, VMEM, VMEM],
        out_specs=VMEM,
        out_shape=pltpu.VMEM((total, shifts, 3, slab, ny, nz), f32),
        compiler_params=limit(20),
        name="powers",
    )(edge, shift_table, shift_ids, own[:2], low[:2], high[:2], slabs, halos)

    here = 4
    spec = pl.BlockSpec((shifts, here, slab, ny, nz), lambda i: (0, i, 0, 0, 0))
    shape = jax.ShapeDtypeStruct((shifts, total, slab, ny, nz), f32)
    return pl.pallas_call(
        final_kernel,
        grid=(total // here,),
        in_specs=[SMEM, SMEM, VMEM, VMEM, VMEM],
        out_specs=[spec, spec],
        out_shape=[shape, shape],
        scratch_shapes=[
            pltpu.VMEM((7 * total, 128), f32),
            pltpu.SMEM((7 * total, 128), f32),
            pltpu.SemaphoreType.DMA,
        ],
        compiler_params=limit(30),
        name="combine",
    )(shift_table, shift_ids, grams, slabs, pltpu.with_memory_space_constraint(powers, pltpu.VMEM))


def solution(mesh):
    placed = (
        P("shift", "dom", None, None),
        P("dom", None, None),
        P("dom", None, None),
        P(),
        P("shift"),
        P(None, "dom", None, None),
    )
    return jax.shard_map(
        lambda *args: tuple(on_device(*args)),
        mesh=mesh,
        in_specs=placed,
        out_specs=(P("shift", None, "dom", None, None), P("shift", None, "dom", None, None)),
        check_vma=False,
    )
```

```python
import functools

import jax
import jax.numpy as jnp
from jax import lax
from jax.experimental import pallas as pl
from jax.experimental.pallas import tpu as pltpu
from jax.sharding import PartitionSpec as P


BOTH = ("dom", "shift")
FIELDS = 10
LEVEL = (0, 1, 1, 2, 2, 2, 3, 3, 3, 3)
POWER = (0, 0, 1, 0, 1, 2, 0, 1, 2, 3)
SIGN = (1.0, -1.0, 1.0, 1.0, -1.0, 1.0, -1.0, 1.0, -1.0, 1.0)
PITCH = 12
BLOCKS = 4
CHUNKS = 4
VMEM = pl.BlockSpec(memory_space=pltpu.VMEM)
SMEM = pl.BlockSpec(memory_space=pltpu.SMEM)


def around(field):
    inner = field[1:-1]
    rows = lax.broadcasted_iota(jnp.int32, inner.shape, 1)
    lanes = lax.broadcasted_iota(jnp.int32, inner.shape, 2)
    ny, nz = inner.shape[1], inner.shape[2]
    total = field[2:] + field[:-2]
    total = total + jnp.where(rows == 0, 0.0, pltpu.roll(inner, 1, 1))
    total = total + jnp.where(rows == ny - 1, 0.0, pltpu.roll(inner, ny - 1, 1))
    total = total + jnp.where(lanes == 0, 0.0, pltpu.roll(inner, 1, 2))
    return total + jnp.where(lanes == nz - 1, 0.0, pltpu.roll(inner, nz - 1, 2))


def masked(field, count, low, high):
    return jnp.concatenate([field[:count] * low, field[count:-count], field[-count:] * high], axis=0)


def ten_fields(w, kappa, q, low, high):
    def p(field, planes):
        cut = (kappa.shape[0] - planes) // 2
        return kappa[cut : cut + planes] * field[1:-1] + around(field)

    slab = w.shape[0] - 6
    e10 = masked(p(w, slab + 4), 2, low, high)
    e01 = q[1:-1] * w[1:-1]
    e20 = masked(p(e10, slab + 2), 1, low, high)
    e11 = masked(p(e01, slab + 2) + q[2:-2] * e10[1:-1], 1, low, high)
    e02 = q[2:-2] * e01[1:-1]
    q3 = q[3:-3]
    e30 = p(e20, slab)
    e21 = p(e11, slab) + q3 * e20[1:-1]
    e12 = p(e02, slab) + q3 * e11[1:-1]
    e03 = q3 * e02[1:-1]
    return (w[3:-3], e10[2:-2], e01[2:-2], e20[1:-1], e11[1:-1], e02[1:-1], e30, e21, e12, e03)


def sketch_kernel(edge, kappa, mass, low, high, wide, sketch, out, held, fld, right, acc0, acc1, cols, sem):
    sources, _, ny, nz = wide.shape
    slab = kappa.shape[0]
    pairs, rows = held.shape[0], held.shape[1]
    chunks = sem.shape[0]
    run = pairs // chunks

    def fetch(c, k):
        return pltpu.make_async_copy(sketch.at[:, k], held.at[k], sem.at[c])

    for c in range(chunks):
        for k in range(run):
            fetch(c, c * run + k).start()

    low_on, high_on = edge[0], edge[1]
    wide_kappa = jnp.concatenate([low[0], kappa[...], high[0]], axis=0)
    q = jnp.concatenate([low[1], mass[...], high[1]], axis=0) - 1.0
    pitch = fld.shape[0] // (FIELDS * sources)

    def one_source(s, carry):
        for f, field in enumerate(ten_fields(wide[s], wide_kappa, q, low_on, high_on)):
            start = pl.multiple_of((f * sources + s) * pitch, 8)
            fld[pl.ds(start, slab * ny), :] = field.reshape(slab * ny, nz)
        return carry

    lax.fori_loop(0, sources, one_source, 0)
    columns = FIELDS * sources
    for k in range(pairs):
        for parity in range(2):
            line = fld[pl.ds(2 * k + parity, columns, stride=pitch), :]
            right[pl.ds(parity * 128, columns), k * nz : (k + 1) * nz] = line.astype(jnp.bfloat16)

    block = 2 * rows // BLOCKS
    for c in range(chunks):
        for k in range(run):
            fetch(c, c * run + k).wait()
        weights = right[:, c * run * nz : (c + 1) * run * nz]
        for b in range(BLOCKS):
            at = slice(b * block, (b + 1) * block)
            left = jnp.concatenate(
                [held[c * run + k, b * block // 2 : (b + 1) * block // 2].reshape(block, nz) for k in range(run)],
                axis=1,
            )
            both = lax.dot_general(left, weights, (((1,), (1,)), ((), ())), preferred_element_type=jnp.float32)
            if c > 0:
                both = both + jnp.concatenate([acc0[at, :], acc1[at, :]], axis=1)
            acc0[at, :] = both[:, :128]
            acc1[at, :] = both[:, 128:]

    strips = rows // 128
    per_piece = strips * sources // out.shape[0]
    for t in range(strips):
        line = acc0[pl.ds(t * 256, 128, stride=2), :] + acc1[pl.ds(t * 256 + 1, 128, stride=2), :]
        cols[t] = line.T
    for t in range(strips):
        for s in range(sources):
            piece = s * (strips // per_piece) + t // per_piece
            place = FIELDS * (t % per_piece)
            out[piece, place : place + FIELDS, :] = cols.at[t][pl.ds(s, FIELDS, stride=sources), :]
    for piece in range(out.shape[0]):
        used = FIELDS * per_piece
        out[piece, used:, :] = jnp.zeros((out.shape[1] - used, 128), jnp.float32)


def gram_kernel(pieces, out):
    rows = pieces[0]
    for peer in range(1, pieces.shape[0]):
        rows = rows + pieces[peer]
    gram = lax.dot_general(
        rows, rows, (((1,), (1,)), ((), ())), preferred_element_type=jnp.float32, precision=lax.Precision.HIGHEST
    )
    gram = gram[:FIELDS, :FIELDS] + gram[FIELDS : 2 * FIELDS, FIELDS : 2 * FIELDS]
    wide = jnp.concatenate([gram, jnp.zeros((FIELDS, 128 - FIELDS), jnp.float32)], axis=1)
    line = wide[0:1]
    for f in range(1, FIELDS):
        line = line + pltpu.roll(wide[f : f + 1], PITCH * f, 1)
    out[...] = jnp.broadcast_to(line[None], out.shape)


def powers_kernel(edge, table, ids, kappa, mass, low, high, *refs):
    *wides, out = refs
    low_on, high_on = edge[0], edge[1]
    wide_kappa = jnp.concatenate([low[0], kappa[...], high[0]], axis=0)
    q = jnp.concatenate([low[1], mass[...], high[1]], axis=0) - 1.0
    shifts = ids.shape[0]
    sigma = [table[ids[j]] for j in range(shifts)]
    here = out.shape[0]
    step = pl.program_id(0)
    base = 0
    for wide in wides:
        count = wide.shape[0] // here

        @pl.when((step >= base) & (step < base + count))
        def _(wide=wide, base=base):
            def one_source(i, carry):
                s = (step - base) * here + i
                w, e10, e01, e20, e11, e02, e30, e21, e12, e03 = ten_fields(wide[s], wide_kappa, q, low_on, high_on)
                out[i, 0] = w
                for j in range(shifts):
                    x = sigma[j]
                    out[i, 3 * j + 1] = x * e01 - e10
                    out[i, 3 * j + 2] = x * (x * e02 - e11) + e20
                    out[i, 3 * j + 3] = x * (x * (x * e03 - e12) + e21) - e30
                return carry

            lax.fori_loop(0, here, one_source, 0)

        base = base + count


def solve_small(gram):
    ridge = 0.001 * (gram[1][1] + gram[2][2] + gram[3][3]) / 3.0 + 1.0
    entry = [[gram[1 + i][1 + k] + (ridge if i == k else 0.0) for k in range(3)] for i in range(3)]
    h = [gram[1 + i][0] for i in range(3)]
    l00 = jnp.sqrt(entry[0][0])
    l10 = entry[1][0] / l00
    l20 = entry[2][0] / l00
    l11 = jnp.sqrt(entry[1][1] - l10 * l10)
    l21 = (entry[2][1] - l20 * l10) / l11
    l22 = jnp.sqrt(entry[2][2] - l20 * l20 - l21 * l21)
    f0 = h[0] / l00
    f1 = (h[1] - l10 * f0) / l11
    f2 = (h[2] - l20 * f0 - l21 * f1) / l22
    c2 = f2 / l22
    c1 = (f1 - l21 * c2) / l11
    c0 = (f0 - l10 * c1 - l20 * c2) / l00
    return c0, c1, c2


def final_kernel(group, table, ids, grams, near, far, sol, res, weights, scalars, sem):
    groups, per_group = 4, near.shape[0]
    shifts = ids.shape[0]
    step = pl.program_id(0)

    @pl.when(step == 0)
    def _():
        parts = grams.shape[0] // (groups * per_group)
        flat = grams.reshape(grams.shape[0], 128)
        lines = []
        for g in range(groups):
            line = None
            for part in range(parts):
                one = flat[pl.ds(part * groups + g, per_group, stride=parts * groups), :]
                line = one if line is None else line + one
            lines.append(line)
        gram = jnp.concatenate(lines, axis=0)
        lane = lax.broadcasted_iota(jnp.int32, gram.shape, 1)
        sigma = jnp.zeros(gram.shape, jnp.float32)
        for j in range(shifts):
            sigma = jnp.where(lane == j, table[ids[j]], sigma)
        terms = {}
        for f in range(FIELDS):
            for e in range(f, FIELDS):
                place = PITCH * f + e
                value = jnp.broadcast_to(gram[:, place : place + 1], gram.shape)
                sign = SIGN[f] * SIGN[e] * (2.0 if LEVEL[f] == LEVEL[e] and f != e else 1.0)
                value = value if sign == 1.0 else value * sign
                key = (LEVEL[f], LEVEL[e], POWER[f] + POWER[e])
                terms[key] = terms[key] + value if key in terms else value
        inner = [[None] * 4 for _ in range(4)]
        for a in range(4):
            for b in range(a, 4):
                value = terms[(a, b, a + b)]
                for power in range(a + b - 1, -1, -1):
                    value = value * sigma + terms[(a, b, power)]
                value = value * (1.0 / 6.0 ** (a + b))
                inner[a][b] = inner[b][a] = value
        center = 6.0 + sigma
        mixed = [[6.0 * inner[i + 1][k] + center * inner[i][k] for k in range(4)] for i in range(3)]
        full = [[None] * 4 for _ in range(4)]
        for i in range(3):
            full[1 + i][0] = mixed[i][0]
            for k in range(3):
                full[1 + i][1 + k] = 6.0 * mixed[i][k + 1] + center * mixed[i][k]
        c0, c1, c2 = solve_small(full)
        rows = gram.shape[0]
        values = (
            c0,
            c1 * (1.0 / 6.0),
            c2 * (1.0 / 36.0),
            1.0 - c0 * center,
            (6.0 * c0 + c1 * center) * (-1.0 / 6.0),
            (6.0 * c1 + c2 * center) * (-1.0 / 36.0),
            c2 * (-1.0 / 36.0),
        )
        for n, value in enumerate(values):
            weights[n * rows : (n + 1) * rows, :] = value
        copy = pltpu.make_async_copy(weights, scalars, sem)
        copy.start()
        copy.wait()

    here = sol.shape[1]
    rows = groups * per_group

    def combine(powers, first):
        for i in range(here):
            s = first + i
            at = lax.rem(group[0] * per_group + step * here + i, rows)
            w = powers[s, 0]
            for j in range(shifts):
                v1, v2, v3 = (powers[s, 3 * j + n] for n in (1, 2, 3))
                c = [scalars[n * rows + at, j] for n in range(7)]
                sol[j, i] = c[0] * w + c[1] * v1 + c[2] * v2
                res[j, i] = c[3] * w + c[4] * v1 + c[5] * v2 + c[6] * v3

    @pl.when(step * here < per_group)
    def _():
        combine(near, step * here)

    @pl.when(step * here >= per_group)
    def _():
        combine(far, 0)


def cost(us):
    return pl.CostEstimate(flops=int(us * 8e6), bytes_accessed=0, transcendentals=0)


def limit(mib):
    return pltpu.CompilerParams(vmem_limit_bytes=mib << 20)


def on_device(sources, kappa, mass, shift_table, shift_ids, sketch):
    f32 = jnp.float32
    dom, shift = lax.axis_size("dom"), lax.axis_size("shift")
    per_group, slab, ny, nz = sources.shape
    total = per_group * shift
    rows = sketch.shape[0]
    pairs = slab * ny // 2
    at = lax.axis_index("dom")
    edge = jnp.stack([at > 0, at < dom - 1]).astype(f32)
    group = lax.axis_index("shift").astype(jnp.int32)[None]

    def planes(cut):
        return jnp.concatenate([kappa[None, cut], mass[None, cut], sources[:, cut]], axis=0)

    low = lax.ppermute(planes(slice(slab - 3, slab)), "dom", [(i, i + 1) for i in range(dom - 1)])
    high = lax.ppermute(planes(slice(0, 3)), "dom", [(i + 1, i) for i in range(dom - 1)])
    wide = jnp.concatenate([low[2:], sources, high[2:]], axis=1)
    from_next = [(i, (i - 1) % shift) for i in range(shift)]
    from_last = [(i, (i + 1) % shift) for i in range(shift)]
    half = per_group // 2
    after = lax.ppermute(wide, "shift", from_next)
    before = lax.ppermute(wide, "shift", from_last)

    held = pltpu.with_memory_space_constraint(sketch.reshape(rows, pairs, 2, nz), pltpu.HBM)
    pieces = pl.pallas_call(
        sketch_kernel,
        in_specs=[SMEM] + [VMEM] * 5 + [pl.BlockSpec(memory_space=pltpu.HBM)],
        out_specs=VMEM,
        out_shape=jax.ShapeDtypeStruct((dom, 24, 128), f32),
        scratch_shapes=[
            pltpu.VMEM((pairs, rows, 2, nz), jnp.bfloat16),
            pltpu.VMEM((FIELDS * per_group * (slab * ny + 8), nz), f32),
            pltpu.VMEM((256, pairs * nz), jnp.bfloat16),
            pltpu.VMEM((2 * rows, 128), f32),
            pltpu.VMEM((2 * rows, 128), f32),
            pltpu.VMEM((rows // 128, 128, 128), f32),
            pltpu.SemaphoreType.DMA((CHUNKS,)),
        ],
        compiler_params=limit(36),
        cost_estimate=cost(12),
        name="sketch_fields",
    )(edge, kappa, mass, low, high, wide, held)
    arrived = lax.all_to_all(pieces, "dom", 0, 0, tiled=True)
    far_first = lax.ppermute(after[:half], "shift", from_next)
    far_last = lax.ppermute(before[half:], "shift", from_last)

    shifts = shift_ids.shape[0]

    def powers_of(name, here, *wides):
        count = sum(array.shape[0] for array in wides)
        shape = (count, 1 + 3 * shifts, slab, ny, nz)
        return pl.pallas_call(
            powers_kernel,
            in_specs=[SMEM, SMEM, SMEM] + [VMEM] * (4 + len(wides)),
            grid=(count // here,),
            out_specs=VMEM if here == count else pl.BlockSpec((here, *shape[1:]), lambda i: (i, 0, 0, 0, 0)),
            out_shape=pltpu.VMEM(shape, f32) if here == count else pltpu.HBM(shape, f32),
            compiler_params=limit(20),
            cost_estimate=cost(count * 0.3),
            name=name,
        )(edge, shift_table, shift_ids, kappa, mass, low, high, *wides)

    near = powers_of("powers_near", per_group, wide)
    lines = pl.pallas_call(
        gram_kernel,
        in_specs=[VMEM],
        out_specs=VMEM,
        out_shape=jax.ShapeDtypeStruct((dom * shift, 1, 128), f32),
        cost_estimate=cost(2),
        name="gram",
    )(arrived)
    grams = lax.all_to_all(lines, BOTH, 0, 0, tiled=True)
    far = powers_of("powers_far", 4, after, far_first, far_last, before)

    here = 4
    steps = total // here

    def place(i, group):
        return (0, lax.rem(group[0] * (per_group // here) + i, steps), 0, 0, 0)

    spec = pl.BlockSpec((shifts, here, slab, ny, nz), place)
    shape = jax.ShapeDtypeStruct((shifts, total, slab, ny, nz), f32)

    def far_place(i, group):
        return (lax.max(i - per_group // here, 0), 0, 0, 0, 0)

    far_spec = pl.BlockSpec((here, *far.shape[1:]), far_place)
    return pl.pallas_call(
        final_kernel,
        grid_spec=pltpu.PrefetchScalarGridSpec(
            num_scalar_prefetch=1,
            grid=(steps,),
            in_specs=[SMEM, SMEM, VMEM, VMEM, far_spec],
            out_specs=[spec, spec],
            scratch_shapes=[
                pltpu.VMEM((7 * total, 128), f32),
                pltpu.SMEM((7 * total, 128), f32),
                pltpu.SemaphoreType.DMA,
            ],
        ),
        out_shape=[shape, shape],
        compiler_params=limit(30),
        name="combine",
    )(
        group,
        shift_table,
        shift_ids,
        grams,
        pltpu.with_memory_space_constraint(near, pltpu.VMEM),
        pltpu.with_memory_space_constraint(far, pltpu.HBM),
    )


def solution(mesh):
    placed = (
        P("shift", "dom", None, None),
        P("dom", None, None),
        P("dom", None, None),
        P(),
        P("shift"),
        P(None, "dom", None, None),
    )
    return jax.shard_map(
        lambda *args: tuple(on_device(*args)),
        mesh=mesh,
        in_specs=placed,
        out_specs=(P("shift", None, "dom", None, None), P("shift", None, "dom", None, None)),
        check_vma=False,
    )
```

```python
import functools

import jax
import jax.numpy as jnp
from jax import lax
from jax.experimental import pallas as pl
from jax.experimental.pallas import tpu as pltpu
from jax.sharding import PartitionSpec as P


BOTH = ("dom", "shift")
FIELDS = 10
LEVEL = (0, 1, 1, 2, 2, 2, 3, 3, 3, 3)
POWER = (0, 0, 1, 0, 1, 2, 0, 1, 2, 3)
SIGN = (1.0, -1.0, 1.0, 1.0, -1.0, 1.0, -1.0, 1.0, -1.0, 1.0)
PITCH = 12
BLOCKS = 4
CHUNKS = 4
VMEM = pl.BlockSpec(memory_space=pltpu.VMEM)
SMEM = pl.BlockSpec(memory_space=pltpu.SMEM)


def around(field):
    inner = field[1:-1]
    rows = lax.broadcasted_iota(jnp.int32, inner.shape, 1)
    lanes = lax.broadcasted_iota(jnp.int32, inner.shape, 2)
    ny, nz = inner.shape[1], inner.shape[2]
    total = field[2:] + field[:-2]
    total = total + jnp.where(rows == 0, 0.0, pltpu.roll(inner, 1, 1))
    total = total + jnp.where(rows == ny - 1, 0.0, pltpu.roll(inner, ny - 1, 1))
    total = total + jnp.where(lanes == 0, 0.0, pltpu.roll(inner, 1, 2))
    return total + jnp.where(lanes == nz - 1, 0.0, pltpu.roll(inner, nz - 1, 2))


def masked(field, count, low, high):
    return jnp.concatenate([field[:count] * low, field[count:-count], field[-count:] * high], axis=0)


def ten_fields(w, kappa, q, low, high):
    def p(field, planes):
        cut = (kappa.shape[0] - planes) // 2
        return kappa[cut : cut + planes] * field[1:-1] + around(field)

    slab = w.shape[0] - 6
    e10 = masked(p(w, slab + 4), 2, low, high)
    e01 = q[1:-1] * w[1:-1]
    e20 = masked(p(e10, slab + 2), 1, low, high)
    e11 = masked(p(e01, slab + 2) + q[2:-2] * e10[1:-1], 1, low, high)
    e02 = q[2:-2] * e01[1:-1]
    q3 = q[3:-3]
    e30 = p(e20, slab)
    e21 = p(e11, slab) + q3 * e20[1:-1]
    e12 = p(e02, slab) + q3 * e11[1:-1]
    e03 = q3 * e02[1:-1]
    return (w[3:-3], e10[2:-2], e01[2:-2], e20[1:-1], e11[1:-1], e02[1:-1], e30, e21, e12, e03)


def edges_kernel(kappa, mass, sources, top, bottom, own, sem):
    slab = kappa.shape[0]
    copies = []
    for out, cut in ((top, pl.ds(slab - 3, 3)), (bottom, pl.ds(0, 3)), (own, pl.ds(0, slab))):
        for source, target in (
            (kappa.at[cut], out.at[0]),
            (mass.at[cut], out.at[1]),
            (sources.at[:, cut], out.at[pl.ds(2, sources.shape[0])]),
        ):
            copies.append(pltpu.make_async_copy(source, target, sem.at[len(copies)]))
    for copy in copies:
        copy.start()
    for copy in copies:
        copy.wait()


def sketch_kernel(edge, low, high, own, sketch, out, near, held, fld, right, acc0, acc1, cols, sem, kept):
    sources = own.shape[0] - 2
    slab, ny, nz = own.shape[1:]
    pairs, rows = held.shape[0], held.shape[1]
    chunks = sem.shape[0]
    run = pairs // chunks

    def fetch(c, k):
        return pltpu.make_async_copy(sketch.at[:, k], held.at[k], sem.at[c])

    for c in range(chunks):
        for k in range(run):
            fetch(c, c * run + k).start()

    low_on, high_on = edge[0], edge[1]
    wide_kappa = jnp.concatenate([low[0], own[0], high[0]], axis=0)
    q = jnp.concatenate([low[1], own[1], high[1]], axis=0) - 1.0
    pitch = fld.shape[0] // (FIELDS * sources)

    def one_source(s, carry):
        wide = jnp.concatenate([low[s + 2], own[s + 2], high[s + 2]], axis=0)
        for f, field in enumerate(ten_fields(wide, wide_kappa, q, low_on, high_on)):
            start = pl.multiple_of((f * sources + s) * pitch, 8)
            fld[pl.ds(start, slab * ny), :] = field.reshape(slab * ny, nz)
        return carry

    lax.fori_loop(0, sources, one_source, 0)
    keep = pltpu.make_async_copy(fld, near, kept)
    keep.start()
    columns = FIELDS * sources
    for k in range(pairs):
        for parity in range(2):
            line = fld[pl.ds(2 * k + parity, columns, stride=pitch), :]
            right[pl.ds(parity * 128, columns), k * nz : (k + 1) * nz] = line.astype(jnp.bfloat16)

    block = 2 * rows // BLOCKS
    for c in range(chunks):
        for k in range(run):
            fetch(c, c * run + k).wait()
        weights = right[:, c * run * nz : (c + 1) * run * nz]
        for b in range(BLOCKS):
            at = slice(b * block, (b + 1) * block)
            left = jnp.concatenate(
                [held[c * run + k, b * block // 2 : (b + 1) * block // 2].reshape(block, nz) for k in range(run)],
                axis=1,
            )
            both = lax.dot_general(left, weights, (((1,), (1,)), ((), ())), preferred_element_type=jnp.float32)
            if c > 0:
                both = both + jnp.concatenate([acc0[at, :], acc1[at, :]], axis=1)
            acc0[at, :] = both[:, :128]
            acc1[at, :] = both[:, 128:]

    strips = rows // 128
    per_piece = strips * sources // out.shape[0]
    for t in range(strips):
        line = acc0[pl.ds(t * 256, 128, stride=2), :] + acc1[pl.ds(t * 256 + 1, 128, stride=2), :]
        cols[t] = line.T
    for t in range(strips):
        for s in range(sources):
            piece = s * (strips // per_piece) + t // per_piece
            place = FIELDS * (t % per_piece)
            out[piece, place : place + FIELDS, :] = cols.at[t][pl.ds(s, FIELDS, stride=sources), :]
    for piece in range(out.shape[0]):
        used = FIELDS * per_piece
        out[piece, used:, :] = jnp.zeros((out.shape[1] - used, 128), jnp.float32)
    keep.wait()


def gram_kernel(pieces, out):
    rows = pieces[0]
    for peer in range(1, pieces.shape[0]):
        rows = rows + pieces[peer]
    gram = lax.dot_general(
        rows, rows, (((1,), (1,)), ((), ())), preferred_element_type=jnp.float32, precision=lax.Precision.HIGHEST
    )
    gram = gram[:FIELDS, :FIELDS] + gram[FIELDS : 2 * FIELDS, FIELDS : 2 * FIELDS]
    wide = jnp.concatenate([gram, jnp.zeros((FIELDS, 128 - FIELDS), jnp.float32)], axis=1)
    line = wide[0:1]
    for f in range(1, FIELDS):
        line = line + pltpu.roll(wide[f : f + 1], PITCH * f, 1)
    out[...] = jnp.broadcast_to(line[None], out.shape)


def load_kernel(_, low, high, after, before, to_after, to_before, sem):
    ends = low.shape[0] - 6
    kept = to_after.shape[0] - 2 * ends
    copies = []
    for out, slab, start in ((to_after, after, 0), (to_before, before, kept)):
        for source, target in (
            (low.at[pl.ds(6, ends)], out.at[pl.ds(0, ends)]),
            (high.at[pl.ds(6, ends)], out.at[pl.ds(ends, ends)]),
            (slab.at[pl.ds(start, kept)], out.at[pl.ds(2 * ends, kept)]),
        ):
            copies.append(pltpu.make_async_copy(source, target, sem.at[len(copies)]))
    for copy in copies:
        copy.start()
    for copy in copies:
        copy.wait()


def far_kernel(parts, outside, edge, kappa, mass, low, high, *refs):
    planes = list(refs[: len(refs) - 1 - len(outside) - bool(outside)])
    out, *held = refs[len(planes) :]
    if outside:
        *held, sem = held
        copies = [pltpu.make_async_copy(planes[n], ref, sem.at[i]) for i, (n, ref) in enumerate(zip(outside, held))]

        @pl.when(pl.program_id(0) == 0)
        def _():
            for copy in copies:
                copy.start()
            for copy in copies:
                copy.wait()

        for n, ref in zip(outside, held):
            planes[n] = ref
    low_on, high_on = edge[0], edge[1]
    wide_kappa = jnp.concatenate([low[0], kappa[...], high[0]], axis=0)
    q = jnp.concatenate([low[1], mass[...], high[1]], axis=0) - 1.0
    slab, ny, nz = kappa.shape
    here = out.shape[0]
    step = pl.program_id(0)
    base = 0
    for count, below, middle, above in parts:

        @pl.when((step >= base) & (step < base + count // here))
        def _(base=base, below=below, middle=middle, above=above):
            def one_source(i, carry):
                s = (step - base) * here + i

                def cut(place, size):
                    ref, first = place
                    return planes[ref][pl.ds(first + s * size, size)]

                wide = jnp.concatenate([cut(below, 3), cut(middle, slab), cut(above, 3)], axis=0)
                for f, field in enumerate(ten_fields(wide, wide_kappa, q, low_on, high_on)):
                    out[i, f] = field.reshape(slab * ny, nz)
                return carry

            lax.fori_loop(0, here, one_source, 0)

        base = base + count // here


def solve_small(gram):
    ridge = 0.001 * (gram[1][1] + gram[2][2] + gram[3][3]) / 3.0 + 1.0
    entry = [[gram[1 + i][1 + k] + (ridge if i == k else 0.0) for k in range(3)] for i in range(3)]
    h = [gram[1 + i][0] for i in range(3)]
    l00 = jnp.sqrt(entry[0][0])
    l10 = entry[1][0] / l00
    l20 = entry[2][0] / l00
    l11 = jnp.sqrt(entry[1][1] - l10 * l10)
    l21 = (entry[2][1] - l20 * l10) / l11
    l22 = jnp.sqrt(entry[2][2] - l20 * l20 - l21 * l21)
    f0 = h[0] / l00
    f1 = (h[1] - l10 * f0) / l11
    f2 = (h[2] - l20 * f0 - l21 * f1) / l22
    c2 = f2 / l22
    c1 = (f1 - l21 * c2) / l11
    c0 = (f0 - l10 * c1 - l20 * c2) / l00
    return c0, c1, c2


def relative_group(step, per):
    place = step // per
    return jnp.where(place == 2, 3, jnp.where(place == 3, 2, place))


def final_kernel(
    group, table, ids, grams, near_hbm, beside_hbm, beyond_hbm, sol, res, near, far, turned, weights, scalars, sem, arrived
):
    groups = 4
    per_group = grams.shape[0] // (groups * groups)
    shifts = ids.shape[0]
    step = pl.program_id(0)
    here = sol.shape[1]
    near_steps = per_group // here
    beside_steps = beside_hbm.shape[0] // here

    def fetch(n):
        if n == 0:
            return pltpu.make_async_copy(near_hbm, near, arrived.at[0])
        source, first = (beside_hbm, 0) if n <= beside_steps else (beyond_hbm, beside_steps)
        taken = source.at[pl.ds((n - 1 - first) * here, here)]
        return pltpu.make_async_copy(taken, far.at[pl.ds((n - 1) * here, here)], arrived.at[n])

    copies = 1 + far.shape[0] // here

    @pl.when(step == 0)
    def _():
        for n in range(copies):
            fetch(n).start()
        parts = grams.shape[0] // (groups * per_group)
        flat = grams.reshape(grams.shape[0], 128)
        lines = []
        for g in range(groups):
            line = None
            for part in range(parts):
                one = flat[pl.ds(part * groups + g, per_group, stride=parts * groups), :]
                line = one if line is None else line + one
            lines.append(line)
        gram = jnp.concatenate(lines, axis=0)
        turned[...] = jnp.concatenate([gram, jnp.zeros((128 - gram.shape[0], 128), jnp.float32)], axis=0).T
        shape = (8, 128)
        line = lax.broadcasted_iota(jnp.int32, shape, 0)
        sigma = jnp.zeros(shape, jnp.float32)
        for j in range(shifts):
            sigma = jnp.where(line == j, table[ids[j]], sigma)
        terms = {}
        for f in range(FIELDS):
            for e in range(f, FIELDS):
                place = PITCH * f + e
                value = jnp.broadcast_to(turned[place : place + 1, :], shape)
                sign = SIGN[f] * SIGN[e] * (2.0 if LEVEL[f] == LEVEL[e] and f != e else 1.0)
                value = value if sign == 1.0 else value * sign
                key = (LEVEL[f], LEVEL[e], POWER[f] + POWER[e])
                terms[key] = terms[key] + value if key in terms else value
        inner = [[None] * 4 for _ in range(4)]
        for a in range(4):
            for b in range(a, 4):
                value = terms[(a, b, a + b)]
                for power in range(a + b - 1, -1, -1):
                    value = value * sigma + terms[(a, b, power)]
                value = value * (1.0 / 6.0 ** (a + b))
                inner[a][b] = inner[b][a] = value
        center = 6.0 + sigma
        mixed = [[6.0 * inner[i + 1][k] + center * inner[i][k] for k in range(4)] for i in range(3)]
        full = [[None] * 4 for _ in range(4)]
        for i in range(3):
            full[1 + i][0] = mixed[i][0]
            for k in range(3):
                full[1 + i][1 + k] = 6.0 * mixed[i][k + 1] + center * mixed[i][k]
        c0, c1, c2 = solve_small(full)
        values = (
            c0,
            c1 * (1.0 / 6.0),
            c2 * (1.0 / 36.0),
            1.0 - c0 * center,
            (6.0 * c0 + c1 * center) * (-1.0 / 6.0),
            (6.0 * c1 + c2 * center) * (-1.0 / 36.0),
            c2 * (-1.0 / 36.0),
        )
        for n, value in enumerate(values):
            weights[8 * n : 8 * (n + 1), :] = value
        copy = pltpu.make_async_copy(weights, scalars, sem)
        copy.start()
        copy.wait()

    ny = sol.shape[3]
    pitch = near.shape[0] // (FIELDS * per_group)
    steps_per_group = per_group // here
    ahead = relative_group(step, steps_per_group)
    first = lax.rem(group[0] + ahead, groups) * per_group + lax.rem(step, steps_per_group) * here

    def combine(read):
        for i in range(here):
            c = [[scalars[8 * n + j, first + i] for n in range(7)] for j in range(shifts)]
            for p in range(sol.shape[2]):
                w, e10, e01, e20, e11, e02, e30, e21, e12, e03 = (read(i, f, p * ny) for f in range(FIELDS))
                for j in range(shifts):
                    x = table[ids[j]]
                    c0, c1, c2, b0, b1, b2, b3 = c[j]
                    v1 = x * e01 - e10
                    v2 = x * (x * e02 - e11) + e20
                    v3 = x * (x * (x * e03 - e12) + e21) - e30
                    sol[j, i, p] = c0 * w + c1 * v1 + c2 * v2
                    res[j, i, p] = b0 * w + b1 * v1 + b2 * v2 + b3 * v3

    @pl.when(step < near_steps)
    def _():
        @pl.when(step == 0)
        def _():
            fetch(0).wait()

        def read(i, f, at):
            return near[pl.ds(pl.multiple_of((f * per_group + step * here + i) * pitch, 8) + at, ny), :]

        combine(read)

    @pl.when(step >= near_steps)
    def _():
        for n in range(1, copies):

            @pl.when(step == near_steps + n - 1)
            def _(n=n):
                fetch(n).wait()

        combine(lambda i, f, at: far[(step - near_steps) * here + i, f, at : at + ny, :])


def cost(us):
    return pl.CostEstimate(flops=int(us * 8e6), bytes_accessed=0, transcendentals=0)


def limit(mib):
    return pltpu.CompilerParams(vmem_limit_bytes=mib << 20)


def on_device(sources, kappa, mass, shift_table, shift_ids, sketch):
    f32 = jnp.float32
    dom, shift = lax.axis_size("dom"), lax.axis_size("shift")
    per_group, slab, ny, nz = sources.shape
    total = per_group * shift
    rows = sketch.shape[0]
    pairs = slab * ny // 2
    at = lax.axis_index("dom")
    edge = jnp.stack([at > 0, at < dom - 1]).astype(f32)
    group = lax.axis_index("shift").astype(jnp.int32)[None]

    HBM = pl.BlockSpec(memory_space=pltpu.HBM)

    def in_hbm(array):
        return pltpu.with_memory_space_constraint(array, pltpu.HBM)

    coeffs = (in_hbm(kappa), in_hbm(mass))
    ends = pltpu.VMEM((2 + per_group, 3, ny, nz), f32)
    top, bottom, own = pl.pallas_call(
        edges_kernel,
        in_specs=[HBM] * 3,
        out_specs=[VMEM] * 3,
        out_shape=[ends, ends, pltpu.VMEM((2 + per_group, slab, ny, nz), f32)],
        scratch_shapes=[pltpu.SemaphoreType.DMA((9,))],
        name="edges",
    )(*coeffs, in_hbm(sources))
    low = lax.ppermute(top, "dom", [(i, i + 1) for i in range(dom - 1)])
    high = lax.ppermute(bottom, "dom", [(i + 1, i) for i in range(dom - 1)])
    from_next = [(i, (i - 1) % shift) for i in range(shift)]
    from_last = [(i, (i + 1) % shift) for i in range(shift)]
    half = per_group // 2
    after = lax.ppermute(sources, "shift", from_next)
    before = lax.ppermute(sources, "shift", from_last)

    pitch = slab * ny + 8
    pieces, near = pl.pallas_call(
        sketch_kernel,
        in_specs=[SMEM] + [VMEM] * 3 + [HBM],
        out_specs=[VMEM, HBM],
        out_shape=[
            pltpu.VMEM((dom, 24, 128), f32),
            pltpu.HBM((FIELDS * per_group * pitch, nz), f32),
        ],
        scratch_shapes=[
            pltpu.VMEM((pairs, rows, 2, nz), jnp.bfloat16),
            pltpu.VMEM((FIELDS * per_group * pitch, nz), f32),
            pltpu.VMEM((256, pairs * nz), jnp.bfloat16),
            pltpu.VMEM((2 * rows, 128), f32),
            pltpu.VMEM((2 * rows, 128), f32),
            pltpu.VMEM((rows // 128, 128, 128), f32),
            pltpu.SemaphoreType.DMA((CHUNKS,)),
            pltpu.SemaphoreType.DMA,
        ],
        compiler_params=limit(36),
        cost_estimate=cost(12),
        name="sketch_fields",
    )(edge, low, high, own, in_hbm(sketch.reshape(rows, pairs, 2, nz)))
    arrived = lax.all_to_all(pieces, "dom", 0, 0, tiled=True)

    def flat(array):
        return array.reshape(-1, ny, nz)

    ends, skip = 3 * per_group, 3 * half
    load = pltpu.VMEM((2 * ends + half * slab, ny, nz), f32)
    load_after, load_before = pl.pallas_call(
        load_kernel,
        in_specs=[HBM] + [pl.BlockSpec(memory_space=pl.ANY)] * 2 + [HBM] * 2,
        out_specs=[VMEM] * 2,
        out_shape=[load, load],
        scratch_shapes=[pltpu.SemaphoreType.DMA((6,))],
        name="load",
    )(near, flat(low), flat(high), in_hbm(flat(after)), in_hbm(flat(before)))
    second_after = lax.ppermute(load_after, "shift", from_next)
    second_before = lax.ppermute(load_before, "shift", from_last)

    def third(array, start):
        return jnp.concatenate([array[start : start + skip], array[ends + start : ends + start + skip]])

    third_after = lax.ppermute(third(second_after, 0), "shift", from_next)
    third_before = lax.ppermute(third(second_before, skip), "shift", from_last)

    here = 4

    def far_fields(parts, outside, *planes):
        count = sum(part[0] for part in parts)
        shape = (count, FIELDS, slab * ny, nz)
        return pl.pallas_call(
            functools.partial(far_kernel, parts, outside),
            in_specs=[SMEM] + [VMEM] * 4 + [HBM if n in outside else VMEM for n in range(len(planes))],
            grid=(count // here,),
            out_specs=pl.BlockSpec((here, *shape[1:]), lambda i: (i, 0, 0, 0)),
            out_shape=pltpu.HBM(shape, f32),
            scratch_shapes=[pltpu.VMEM(planes[n].shape, f32) for n in outside]
            + [pltpu.SemaphoreType.DMA((len(outside),))] * bool(outside),
            compiler_params=limit(20),
            cost_estimate=cost(count * 0.3),
        )(edge, kappa, mass, low, high, *planes)

    lines = pl.pallas_call(
        gram_kernel,
        in_specs=[VMEM],
        out_specs=VMEM,
        out_shape=pltpu.VMEM((dom * shift, 1, 128), f32),
        cost_estimate=cost(2),
        name="gram",
    )(pltpu.with_memory_space_constraint(arrived, pltpu.VMEM))
    grams = lax.all_to_all(lines, BOTH, 0, 0, tiled=True)
    beside = far_fields(
        ((per_group, (0, 0), (1, 0), (0, ends)), (per_group, (2, 0), (3, 0), (2, ends))),
        (1, 3),
        second_after, in_hbm(flat(after)), second_before, in_hbm(flat(before)),
    )
    beyond = far_fields(
        ((half, (0, 0), (1, 2 * ends), (0, skip)), (half, (2, 0), (3, 2 * ends), (2, skip))),
        (),
        third_after, second_after, third_before, second_before,
    )

    here = per_group
    steps = total // here
    shifts = shift_ids.shape[0]
    per = per_group // here

    def place(i, group):
        return (0, lax.rem(group[0] + relative_group(i, per), shift) * per + lax.rem(i, per), 0, 0, 0)

    spec = pl.BlockSpec((shifts, here, slab, ny, nz), place)
    shape = jax.ShapeDtypeStruct((shifts, total, slab, ny, nz), f32)
    return pl.pallas_call(
        final_kernel,
        grid_spec=pltpu.PrefetchScalarGridSpec(
            num_scalar_prefetch=1,
            grid=(steps,),
            in_specs=[SMEM, SMEM, VMEM, HBM, HBM, HBM],
            out_specs=[spec, spec],
            scratch_shapes=[
                pltpu.VMEM(near.shape, f32),
                pltpu.VMEM((total - per_group, FIELDS, slab * ny, nz), f32),
                pltpu.VMEM((128, 128), f32),
                pltpu.VMEM((56, 128), f32),
                pltpu.SMEM((56, 128), f32),
                pltpu.SemaphoreType.DMA,
                pltpu.SemaphoreType.DMA((1 + (total - per_group) // here,)),
            ],
        ),
        out_shape=[shape, shape],
        compiler_params=limit(36),
        name="combine",
    )(group, shift_table, shift_ids, grams, in_hbm(near), in_hbm(beside), in_hbm(beyond))


def solution(mesh):
    placed = (
        P("shift", "dom", None, None),
        P("dom", None, None),
        P("dom", None, None),
        P(),
        P("shift"),
        P(None, "dom", None, None),
    )

    def body(*args):
        return tuple(on_device(*args))

    return jax.shard_map(
        body,
        mesh=mesh,
        in_specs=placed,
        out_specs=(P("shift", None, "dom", None, None), P("shift", None, "dom", None, None)),
        check_vma=False,
    )
```

```python
import functools

import jax
import jax.numpy as jnp
from jax import lax
from jax.experimental import pallas as pl
from jax.experimental.pallas import tpu as pltpu
from jax.sharding import PartitionSpec as P


BOTH = ("dom", "shift")
FIELDS = 10
LEVEL = (0, 1, 1, 2, 2, 2, 3, 3, 3, 3)
POWER = (0, 0, 1, 0, 1, 2, 0, 1, 2, 3)
SIGN = (1.0, -1.0, 1.0, 1.0, -1.0, 1.0, -1.0, 1.0, -1.0, 1.0)
PITCH = 12
BLOCKS = 4
CHUNKS = 4
VMEM = pl.BlockSpec(memory_space=pltpu.VMEM)
SMEM = pl.BlockSpec(memory_space=pltpu.SMEM)


def around(field):
    inner = field[1:-1]
    rows = lax.broadcasted_iota(jnp.int32, inner.shape, 1)
    lanes = lax.broadcasted_iota(jnp.int32, inner.shape, 2)
    ny, nz = inner.shape[1], inner.shape[2]
    total = field[2:] + field[:-2]
    total = total + jnp.where(rows == 0, 0.0, pltpu.roll(inner, 1, 1))
    total = total + jnp.where(rows == ny - 1, 0.0, pltpu.roll(inner, ny - 1, 1))
    total = total + jnp.where(lanes == 0, 0.0, pltpu.roll(inner, 1, 2))
    return total + jnp.where(lanes == nz - 1, 0.0, pltpu.roll(inner, nz - 1, 2))


def masked(field, count, low, high):
    return jnp.concatenate([field[:count] * low, field[count:-count], field[-count:] * high], axis=0)


def ten_fields(w, kappa, q, low, high):
    def p(field, planes):
        cut = (kappa.shape[0] - planes) // 2
        return kappa[cut : cut + planes] * field[1:-1] + around(field)

    slab = w.shape[0] - 6
    e10 = masked(p(w, slab + 4), 2, low, high)
    e01 = q[1:-1] * w[1:-1]
    e20 = masked(p(e10, slab + 2), 1, low, high)
    e11 = masked(p(e01, slab + 2) + q[2:-2] * e10[1:-1], 1, low, high)
    e02 = q[2:-2] * e01[1:-1]
    q3 = q[3:-3]
    e30 = p(e20, slab)
    e21 = p(e11, slab) + q3 * e20[1:-1]
    e12 = p(e02, slab) + q3 * e11[1:-1]
    e03 = q3 * e02[1:-1]
    return (w[3:-3], e10[2:-2], e01[2:-2], e20[1:-1], e11[1:-1], e02[1:-1], e30, e21, e12, e03)


def edges_kernel(kappa, mass, sources, top, bottom, own, sem):
    slab = kappa.shape[0]
    copies = []
    for out, cut in ((top, pl.ds(slab - 3, 3)), (bottom, pl.ds(0, 3)), (own, pl.ds(0, slab))):
        for source, target in (
            (kappa.at[cut], out.at[0]),
            (mass.at[cut], out.at[1]),
            (sources.at[:, cut], out.at[pl.ds(2, sources.shape[0])]),
        ):
            copies.append(pltpu.make_async_copy(source, target, sem.at[len(copies)]))
    for copy in copies:
        copy.start()
    for copy in copies:
        copy.wait()


def sketch_kernel(edge, low, high, own, sketch, out, near, held, fld, right, acc0, acc1, cols, sem, kept):
    sources = own.shape[0] - 2
    slab, ny, nz = own.shape[1:]
    pairs, rows = held.shape[0], held.shape[1]
    chunks = sem.shape[0]
    run = pairs // chunks

    def fetch(c, k):
        return pltpu.make_async_copy(sketch.at[:, k], held.at[k], sem.at[c])

    for c in range(chunks):
        for k in range(run):
            fetch(c, c * run + k).start()

    low_on, high_on = edge[0], edge[1]
    wide_kappa = jnp.concatenate([low[0], own[0], high[0]], axis=0)
    q = jnp.concatenate([low[1], own[1], high[1]], axis=0) - 1.0
    pitch = fld.shape[0] // (FIELDS * sources)

    def one_source(s, carry):
        wide = jnp.concatenate([low[s + 2], own[s + 2], high[s + 2]], axis=0)
        for f, field in enumerate(ten_fields(wide, wide_kappa, q, low_on, high_on)):
            start = pl.multiple_of((f * sources + s) * pitch, 8)
            fld[pl.ds(start, slab * ny), :] = field.reshape(slab * ny, nz)
        return carry

    lax.fori_loop(0, sources, one_source, 0)
    keep = pltpu.make_async_copy(fld, near, kept)
    keep.start()
    columns = FIELDS * sources
    for k in range(pairs):
        for parity in range(2):
            line = fld[pl.ds(2 * k + parity, columns, stride=pitch), :]
            right[pl.ds(parity * 128, columns), k * nz : (k + 1) * nz] = line.astype(jnp.bfloat16)

    block = 2 * rows // BLOCKS
    for c in range(chunks):
        for k in range(run):
            fetch(c, c * run + k).wait()
        weights = right[:, c * run * nz : (c + 1) * run * nz]
        for b in range(BLOCKS):
            at = slice(b * block, (b + 1) * block)
            left = jnp.concatenate(
                [held[c * run + k, b * block // 2 : (b + 1) * block // 2].reshape(block, nz) for k in range(run)],
                axis=1,
            )
            both = lax.dot_general(left, weights, (((1,), (1,)), ((), ())), preferred_element_type=jnp.float32)
            if c > 0:
                both = both + jnp.concatenate([acc0[at, :], acc1[at, :]], axis=1)
            acc0[at, :] = both[:, :128]
            acc1[at, :] = both[:, 128:]

    strips = rows // 128
    per_piece = strips * sources // out.shape[0]
    for t in range(strips):
        line = acc0[pl.ds(t * 256, 128, stride=2), :] + acc1[pl.ds(t * 256 + 1, 128, stride=2), :]
        cols[t] = line.T
    for t in range(strips):
        for s in range(sources):
            piece = s * (strips // per_piece) + t // per_piece
            place = FIELDS * (t % per_piece)
            out[piece, place : place + FIELDS, :] = cols.at[t][pl.ds(s, FIELDS, stride=sources), :]
    for piece in range(out.shape[0]):
        used = FIELDS * per_piece
        out[piece, used:, :] = jnp.zeros((out.shape[1] - used, 128), jnp.float32)
    keep.wait()


def gram_kernel(pieces, out):
    rows = pieces[0]
    for peer in range(1, pieces.shape[0]):
        rows = rows + pieces[peer]
    gram = lax.dot_general(
        rows, rows, (((1,), (1,)), ((), ())), preferred_element_type=jnp.float32, precision=lax.Precision.HIGHEST
    )
    gram = gram[:FIELDS, :FIELDS] + gram[FIELDS : 2 * FIELDS, FIELDS : 2 * FIELDS]
    wide = jnp.concatenate([gram, jnp.zeros((FIELDS, 128 - FIELDS), jnp.float32)], axis=1)
    line = wide[0:1]
    for f in range(1, FIELDS):
        line = line + pltpu.roll(wide[f : f + 1], PITCH * f, 1)
    out[...] = jnp.broadcast_to(line[None], out.shape)


def load_kernel(_, low, high, after, before, to_after, to_before, sem):
    ends = low.shape[0] - 6
    kept = to_after.shape[0] - 2 * ends
    copies = []
    for out, slab, start in ((to_after, after, 0), (to_before, before, kept)):
        for source, target in (
            (low.at[pl.ds(6, ends)], out.at[pl.ds(0, ends)]),
            (high.at[pl.ds(6, ends)], out.at[pl.ds(ends, ends)]),
            (slab.at[pl.ds(start, kept)], out.at[pl.ds(2 * ends, kept)]),
        ):
            copies.append(pltpu.make_async_copy(source, target, sem.at[len(copies)]))
    for copy in copies:
        copy.start()
    for copy in copies:
        copy.wait()


def wide_coefficients(kappa, mass, low, high):
    return jnp.concatenate([low[0], kappa, high[0]], axis=0), jnp.concatenate([low[1], mass, high[1]], axis=0) - 1.0


def fields_to(out, planes, places, s, wide_kappa, q, low_on, high_on):
    slab = wide_kappa.shape[0] - 6
    parts = []
    for (ref, first), size in zip(places, (3, slab, 3)):
        parts.append(planes[ref][pl.ds(first + s * size, size)])
    for f, field in enumerate(ten_fields(jnp.concatenate(parts, axis=0), wide_kappa, q, low_on, high_on)):
        out[f] = field.reshape(-1, field.shape[2])


def far_kernel(sections, edge, kappa, mass, low, high, halo_after, halo_before, after, before, out, *held):
    *held, sem = held
    here = out.shape[0]
    step = pl.program_id(0)
    copies = [pltpu.make_async_copy(*pair, sem.at[n]) for n, pair in enumerate(zip((after, before), held))]

    @pl.when(step == 0)
    def _():
        for copy in copies:
            copy.start()

    wide_kappa, q = wide_coefficients(kappa[...], mass[...], low, high)
    base = 0
    for (count, *places), copy in zip(sections, copies):

        @pl.when(step == base)
        def _(copy=copy):
            copy.wait()

        @pl.when((step >= base) & (step < base + count // here))
        def _(base=base, places=places):
            def one_source(i, carry):
                s = (step - base) * here + i
                planes = (halo_after, held[0], halo_before, held[1])
                fields_to(out.at[i], planes, places, s, wide_kappa, q, edge[0], edge[1])
                return carry

            lax.fori_loop(0, here, one_source, 0)

        base = base + count // here


def solve_small(gram):
    ridge = 0.001 * (gram[1][1] + gram[2][2] + gram[3][3]) / 3.0 + 1.0
    entry = [[gram[1 + i][1 + k] + (ridge if i == k else 0.0) for k in range(3)] for i in range(3)]
    h = [gram[1 + i][0] for i in range(3)]
    l00 = jnp.sqrt(entry[0][0])
    l10 = entry[1][0] / l00
    l20 = entry[2][0] / l00
    l11 = jnp.sqrt(entry[1][1] - l10 * l10)
    l21 = (entry[2][1] - l20 * l10) / l11
    l22 = jnp.sqrt(entry[2][2] - l20 * l20 - l21 * l21)
    f0 = h[0] / l00
    f1 = (h[1] - l10 * f0) / l11
    f2 = (h[2] - l20 * f0 - l21 * f1) / l22
    c2 = f2 / l22
    c1 = (f1 - l21 * c2) / l11
    c0 = (f0 - l10 * c1 - l20 * c2) / l00
    return c0, c1, c2


def relative_group(step, per):
    place = step // per
    return jnp.where(place == 2, 3, jnp.where(place == 3, 2, place))


def final_kernel(
    sections, group, table, ids, edge, kappa, mass, low, high, third_after, second_after, third_before, second_before,
    grams, near_hbm, beside_hbm, sol, res, near, far, turned, weights, scalars, sem, arrived,
):
    groups = 4
    per_group = grams.shape[0] // (groups * groups)
    shifts = ids.shape[0]
    step = pl.program_id(0)
    here = sol.shape[1]
    near_steps = per_group // here
    beside_steps = beside_hbm.shape[0] // here

    def fetch(n):
        if n == 0:
            return pltpu.make_async_copy(near_hbm, near, arrived.at[0])
        rows = pl.ds((n - 1) * here, here)
        return pltpu.make_async_copy(beside_hbm.at[rows], far.at[rows], arrived.at[n])

    copies = 1 + beside_steps

    @pl.when(step == 0)
    def _():
        for n in range(copies):
            fetch(n).start()
        parts = grams.shape[0] // (groups * per_group)
        flat = grams.reshape(grams.shape[0], 128)
        lines = []
        for g in range(groups):
            line = None
            for part in range(parts):
                one = flat[pl.ds(part * groups + g, per_group, stride=parts * groups), :]
                line = one if line is None else line + one
            lines.append(line)
        gram = jnp.concatenate(lines, axis=0)
        turned[...] = jnp.concatenate([gram, jnp.zeros((128 - gram.shape[0], 128), jnp.float32)], axis=0).T
        shape = (8, 128)
        line = lax.broadcasted_iota(jnp.int32, shape, 0)
        sigma = jnp.zeros(shape, jnp.float32)
        for j in range(shifts):
            sigma = jnp.where(line == j, table[ids[j]], sigma)
        terms = {}
        for f in range(FIELDS):
            for e in range(f, FIELDS):
                place = PITCH * f + e
                value = jnp.broadcast_to(turned[place : place + 1, :], shape)
                sign = SIGN[f] * SIGN[e] * (2.0 if LEVEL[f] == LEVEL[e] and f != e else 1.0)
                value = value if sign == 1.0 else value * sign
                key = (LEVEL[f], LEVEL[e], POWER[f] + POWER[e])
                terms[key] = terms[key] + value if key in terms else value
        inner = [[None] * 4 for _ in range(4)]
        for a in range(4):
            for b in range(a, 4):
                value = terms[(a, b, a + b)]
                for power in range(a + b - 1, -1, -1):
                    value = value * sigma + terms[(a, b, power)]
                value = value * (1.0 / 6.0 ** (a + b))
                inner[a][b] = inner[b][a] = value
        center = 6.0 + sigma
        mixed = [[6.0 * inner[i + 1][k] + center * inner[i][k] for k in range(4)] for i in range(3)]
        full = [[None] * 4 for _ in range(4)]
        for i in range(3):
            full[1 + i][0] = mixed[i][0]
            for k in range(3):
                full[1 + i][1 + k] = 6.0 * mixed[i][k + 1] + center * mixed[i][k]
        c0, c1, c2 = solve_small(full)
        values = (
            c0,
            c1 * (1.0 / 6.0),
            c2 * (1.0 / 36.0),
            1.0 - c0 * center,
            (6.0 * c0 + c1 * center) * (-1.0 / 6.0),
            (6.0 * c1 + c2 * center) * (-1.0 / 36.0),
            c2 * (-1.0 / 36.0),
        )
        for n, value in enumerate(values):
            weights[8 * n : 8 * (n + 1), :] = value
        copy = pltpu.make_async_copy(weights, scalars, sem)
        copy.start()
        wide_kappa, q = wide_coefficients(kappa[...], mass[...], low, high)
        planes = (third_after, second_after, third_before, second_before)
        base = beside_hbm.shape[0]
        for count, *places in sections:

            def one_source(s, carry, base=base, places=places):
                fields_to(far.at[base + s], planes, places, s, wide_kappa, q, edge[0], edge[1])
                return carry

            lax.fori_loop(0, count, one_source, 0)
            base = base + count
        copy.wait()

    ny = sol.shape[3]
    pitch = near.shape[0] // (FIELDS * per_group)
    steps_per_group = per_group // here
    ahead = relative_group(step, steps_per_group)
    first = lax.rem(group[0] + ahead, groups) * per_group + lax.rem(step, steps_per_group) * here

    def combine(read):
        for i in range(here):
            c = [[scalars[8 * n + j, first + i] for n in range(7)] for j in range(shifts)]
            for p in range(sol.shape[2]):
                w, e10, e01, e20, e11, e02, e30, e21, e12, e03 = (read(i, f, p * ny) for f in range(FIELDS))
                for j in range(shifts):
                    x = table[ids[j]]
                    c0, c1, c2, b0, b1, b2, b3 = c[j]
                    v1 = x * e01 - e10
                    v2 = x * (x * e02 - e11) + e20
                    v3 = x * (x * (x * e03 - e12) + e21) - e30
                    sol[j, i, p] = c0 * w + c1 * v1 + c2 * v2
                    res[j, i, p] = b0 * w + b1 * v1 + b2 * v2 + b3 * v3

    @pl.when(step < near_steps)
    def _():
        @pl.when(step == 0)
        def _():
            fetch(0).wait()

        def read(i, f, at):
            return near[pl.ds(pl.multiple_of((f * per_group + step * here + i) * pitch, 8) + at, ny), :]

        combine(read)

    @pl.when(step >= near_steps)
    def _():
        for n in range(1, copies):

            @pl.when(step == near_steps + n - 1)
            def _(n=n):
                fetch(n).wait()

        combine(lambda i, f, at: far[(step - near_steps) * here + i, f, at : at + ny, :])


def cost(us):
    return pl.CostEstimate(flops=int(us * 8e6), bytes_accessed=0, transcendentals=0)


def limit(mib):
    return pltpu.CompilerParams(vmem_limit_bytes=mib << 20)


def on_device(sources, kappa, mass, shift_table, shift_ids, sketch):
    f32 = jnp.float32
    dom, shift = lax.axis_size("dom"), lax.axis_size("shift")
    per_group, slab, ny, nz = sources.shape
    total = per_group * shift
    rows = sketch.shape[0]
    pairs = slab * ny // 2
    at = lax.axis_index("dom")
    edge = jnp.stack([at > 0, at < dom - 1]).astype(f32)
    group = lax.axis_index("shift").astype(jnp.int32)[None]

    HBM = pl.BlockSpec(memory_space=pltpu.HBM)

    def in_hbm(array):
        return pltpu.with_memory_space_constraint(array, pltpu.HBM)

    coeffs = (in_hbm(kappa), in_hbm(mass))
    ends = pltpu.VMEM((2 + per_group, 3, ny, nz), f32)
    top, bottom, own = pl.pallas_call(
        edges_kernel,
        in_specs=[HBM] * 3,
        out_specs=[VMEM] * 3,
        out_shape=[ends, ends, pltpu.VMEM((2 + per_group, slab, ny, nz), f32)],
        scratch_shapes=[pltpu.SemaphoreType.DMA((9,))],
        name="edges",
    )(*coeffs, in_hbm(sources))
    low = lax.ppermute(top, "dom", [(i, i + 1) for i in range(dom - 1)])
    high = lax.ppermute(bottom, "dom", [(i + 1, i) for i in range(dom - 1)])
    from_next = [(i, (i - 1) % shift) for i in range(shift)]
    from_last = [(i, (i + 1) % shift) for i in range(shift)]
    half = per_group // 2
    after = lax.ppermute(sources, "shift", from_next)
    before = lax.ppermute(sources, "shift", from_last)

    pitch = slab * ny + 8
    pieces, near = pl.pallas_call(
        sketch_kernel,
        in_specs=[SMEM] + [VMEM] * 3 + [HBM],
        out_specs=[VMEM, HBM],
        out_shape=[
            pltpu.VMEM((dom, 24, 128), f32),
            pltpu.HBM((FIELDS * per_group * pitch, nz), f32),
        ],
        scratch_shapes=[
            pltpu.VMEM((pairs, rows, 2, nz), jnp.bfloat16),
            pltpu.VMEM((FIELDS * per_group * pitch, nz), f32),
            pltpu.VMEM((256, pairs * nz), jnp.bfloat16),
            pltpu.VMEM((2 * rows, 128), f32),
            pltpu.VMEM((2 * rows, 128), f32),
            pltpu.VMEM((rows // 128, 128, 128), f32),
            pltpu.SemaphoreType.DMA((CHUNKS,)),
            pltpu.SemaphoreType.DMA,
        ],
        compiler_params=limit(36),
        cost_estimate=cost(12),
        name="sketch_fields",
    )(edge, low, high, own, in_hbm(sketch.reshape(rows, pairs, 2, nz)))
    arrived = lax.all_to_all(pieces, "dom", 0, 0, tiled=True)

    def flat(array):
        return array.reshape(-1, ny, nz)

    ends, skip = 3 * per_group, 3 * half
    load = pltpu.VMEM((2 * ends + half * slab, ny, nz), f32)
    load_after, load_before = pl.pallas_call(
        load_kernel,
        in_specs=[HBM] + [pl.BlockSpec(memory_space=pl.ANY)] * 2 + [HBM] * 2,
        out_specs=[VMEM] * 2,
        out_shape=[load, load],
        scratch_shapes=[pltpu.SemaphoreType.DMA((6,))],
        name="load",
    )(near, flat(low), flat(high), in_hbm(flat(after)), in_hbm(flat(before)))
    second_after = lax.ppermute(load_after, "shift", from_next)
    second_before = lax.ppermute(load_before, "shift", from_last)

    def third(array, start):
        return jnp.concatenate([array[start : start + skip], array[ends + start : ends + start + skip]])

    third_after = lax.ppermute(third(second_after, 0), "shift", from_next)
    third_before = lax.ppermute(third(second_before, skip), "shift", from_last)

    lines = pl.pallas_call(
        gram_kernel,
        in_specs=[VMEM],
        out_specs=VMEM,
        out_shape=pltpu.VMEM((dom * shift, 1, 128), f32),
        cost_estimate=cost(2),
        name="gram",
    )(pltpu.with_memory_space_constraint(arrived, pltpu.VMEM))
    grams = lax.all_to_all(lines, BOTH, 0, 0, tiled=True)
    far_here = 4
    far_shape = (2 * per_group, FIELDS, slab * ny, nz)
    slabs = pltpu.VMEM((per_group * slab, ny, nz), f32)
    beside = pl.pallas_call(
        functools.partial(
            far_kernel,
            ((per_group, (0, 0), (1, 0), (0, ends)), (per_group, (2, 0), (3, 0), (2, ends))),
        ),
        in_specs=[SMEM] + [VMEM] * 6 + [HBM] * 2,
        grid=(far_shape[0] // far_here,),
        out_specs=pl.BlockSpec((far_here, *far_shape[1:]), lambda i: (i, 0, 0, 0)),
        out_shape=pltpu.HBM(far_shape, f32),
        scratch_shapes=[slabs, slabs, pltpu.SemaphoreType.DMA((2,))],
        compiler_params=limit(20),
        cost_estimate=cost(6),
        name="fields_beside",
    )(edge, kappa, mass, low, high, second_after, second_before, in_hbm(flat(after)), in_hbm(flat(before)))
    sections = (
        (half, (0, 0), (1, 2 * ends), (0, skip)),
        (half, (2, 0), (3, 2 * ends), (2, skip)),
    )

    here = per_group
    steps = total // here
    shifts = shift_ids.shape[0]
    per = per_group // here

    def place(i, group):
        return (0, lax.rem(group[0] + relative_group(i, per), shift) * per + lax.rem(i, per), 0, 0, 0)

    spec = pl.BlockSpec((shifts, here, slab, ny, nz), place)
    shape = jax.ShapeDtypeStruct((shifts, total, slab, ny, nz), f32)
    return pl.pallas_call(
        functools.partial(final_kernel, sections),
        grid_spec=pltpu.PrefetchScalarGridSpec(
            num_scalar_prefetch=1,
            grid=(steps,),
            in_specs=[SMEM] * 3 + [VMEM] * 9 + [HBM] * 2,
            out_specs=[spec, spec],
            scratch_shapes=[
                pltpu.VMEM(near.shape, f32),
                pltpu.VMEM((total - per_group, FIELDS, slab * ny, nz), f32),
                pltpu.VMEM((128, 128), f32),
                pltpu.VMEM((56, 128), f32),
                pltpu.SMEM((56, 128), f32),
                pltpu.SemaphoreType.DMA,
                pltpu.SemaphoreType.DMA((1 + far_shape[0] // here,)),
            ],
        ),
        out_shape=[shape, shape],
        compiler_params=limit(36),
        name="combine",
    )(
        group, shift_table, shift_ids, edge, kappa, mass, low, high,
        third_after, second_after, third_before, second_before,
        grams, in_hbm(near), in_hbm(beside),
    )


def solution(mesh):
    placed = (
        P("shift", "dom", None, None),
        P("dom", None, None),
        P("dom", None, None),
        P(),
        P("shift"),
        P(None, "dom", None, None),
    )

    def body(*args):
        return tuple(on_device(*args))

    return jax.shard_map(
        body,
        mesh=mesh,
        in_specs=placed,
        out_specs=(P("shift", None, "dom", None, None), P("shift", None, "dom", None, None)),
        check_vma=False,
    )
```

```python
import functools

import jax
import jax.numpy as jnp
from jax import lax
from jax.experimental import pallas as pl
from jax.experimental.pallas import tpu as pltpu
from jax.sharding import PartitionSpec as P


BOTH = ("dom", "shift")
FIELDS = 10
LEVEL = (0, 1, 1, 2, 2, 2, 3, 3, 3, 3)
POWER = (0, 0, 1, 0, 1, 2, 0, 1, 2, 3)
SIGN = (1.0, -1.0, 1.0, 1.0, -1.0, 1.0, -1.0, 1.0, -1.0, 1.0)
PITCH = 12
BLOCKS = 4
CHUNKS = 4
VMEM = pl.BlockSpec(memory_space=pltpu.VMEM)
SMEM = pl.BlockSpec(memory_space=pltpu.SMEM)


def around(field):
    inner = field[1:-1]
    lanes = lax.broadcasted_iota(jnp.int32, inner.shape, 2)
    nz = inner.shape[2]
    total = field[2:] + field[:-2]
    edge = jnp.zeros((inner.shape[0], 1, nz), jnp.float32)
    total = total + jnp.concatenate([edge, inner[:, :-1]], axis=1) + jnp.concatenate([inner[:, 1:], edge], axis=1)
    total = total + jnp.where(lanes == 0, 0.0, pltpu.roll(inner, 1, 2))
    return total + jnp.where(lanes == nz - 1, 0.0, pltpu.roll(inner, nz - 1, 2))


def masked(field, count, low, high):
    return jnp.concatenate([field[:count] * low, field[count:-count], field[-count:] * high], axis=0)


def ten_fields(w, kappa, q, low, high):
    def p(field, planes):
        cut = (kappa.shape[0] - planes) // 2
        return kappa[cut : cut + planes] * field[1:-1] + around(field)

    slab = w.shape[0] - 6
    e10 = masked(p(w, slab + 4), 2, low, high)
    e01 = q[1:-1] * w[1:-1]
    e20 = masked(p(e10, slab + 2), 1, low, high)
    e11 = masked(p(e01, slab + 2) + q[2:-2] * e10[1:-1], 1, low, high)
    e02 = q[2:-2] * e01[1:-1]
    q3 = q[3:-3]
    e30 = p(e20, slab)
    e21 = p(e11, slab) + q3 * e20[1:-1]
    e12 = p(e02, slab) + q3 * e11[1:-1]
    e03 = q3 * e02[1:-1]
    return (w[3:-3], e10[2:-2], e01[2:-2], e20[1:-1], e11[1:-1], e02[1:-1], e30, e21, e12, e03)


def edges_kernel(kappa, mass, sources, top, bottom, own, sem):
    slab = kappa.shape[0]
    copies = []
    for out, cut in ((top, pl.ds(slab - 3, 3)), (bottom, pl.ds(0, 3)), (own, pl.ds(0, slab))):
        for source, target in (
            (kappa.at[cut], out.at[0]),
            (mass.at[cut], out.at[1]),
            (sources.at[:, cut], out.at[pl.ds(2, sources.shape[0])]),
        ):
            copies.append(pltpu.make_async_copy(source, target, sem.at[len(copies)]))
    for copy in copies:
        copy.start()
    for copy in copies:
        copy.wait()


def sketch_kernel(edge, low, high, own, sketch, out, near, held, fld, right, acc0, acc1, cols, sem, kept):
    sources = own.shape[0] - 2
    slab, ny, nz = own.shape[1:]
    pairs, rows = held.shape[0], held.shape[1]
    chunks = sem.shape[0]
    run = pairs // chunks

    def fetch(c, k):
        return pltpu.make_async_copy(sketch.at[:, k], held.at[k], sem.at[c])

    for c in range(chunks):
        for k in range(run):
            fetch(c, c * run + k).start()

    low_on, high_on = edge[0], edge[1]
    wide_kappa = jnp.concatenate([low[0], own[0], high[0]], axis=0)
    q = jnp.concatenate([low[1], own[1], high[1]], axis=0) - 1.0
    pitch = fld.shape[0] // (FIELDS * sources)

    def one_source(s, carry):
        wide = jnp.concatenate([low[s + 2], own[s + 2], high[s + 2]], axis=0)
        for f, field in enumerate(ten_fields(wide, wide_kappa, q, low_on, high_on)):
            start = pl.multiple_of((f * sources + s) * pitch, 8)
            fld[pl.ds(start, slab * ny), :] = field.reshape(slab * ny, nz)
        return carry

    lax.fori_loop(0, sources, one_source, 0)
    keep = pltpu.make_async_copy(fld, near, kept)
    keep.start()
    columns = FIELDS * sources
    for k in range(pairs):
        for parity in range(2):
            line = fld[pl.ds(2 * k + parity, columns, stride=pitch), :]
            right[pl.ds(parity * 128, columns), k * nz : (k + 1) * nz] = line.astype(jnp.bfloat16)

    block = 2 * rows // BLOCKS
    for c in range(chunks):
        for k in range(run):
            fetch(c, c * run + k).wait()
        weights = right[:, c * run * nz : (c + 1) * run * nz]
        for b in range(BLOCKS):
            at = slice(b * block, (b + 1) * block)
            left = jnp.concatenate(
                [held[c * run + k, b * block // 2 : (b + 1) * block // 2].reshape(block, nz) for k in range(run)],
                axis=1,
            )
            both = lax.dot_general(left, weights, (((1,), (1,)), ((), ())), preferred_element_type=jnp.float32)
            if c > 0:
                both = both + jnp.concatenate([acc0[at, :], acc1[at, :]], axis=1)
            acc0[at, :] = both[:, :128]
            acc1[at, :] = both[:, 128:]

    strips = rows // 128
    per_piece = strips * sources // out.shape[0]
    for t in range(strips):
        line = acc0[pl.ds(t * 256, 128, stride=2), :] + acc1[pl.ds(t * 256 + 1, 128, stride=2), :]
        cols[t] = line.T
    for t in range(strips):
        for s in range(sources):
            piece = s * (strips // per_piece) + t // per_piece
            place = FIELDS * (t % per_piece)
            out[piece, place : place + FIELDS, :] = cols.at[t][pl.ds(s, FIELDS, stride=sources), :]
    for piece in range(out.shape[0]):
        used = FIELDS * per_piece
        out[piece, used:, :] = jnp.zeros((out.shape[1] - used, 128), jnp.float32)
    keep.wait()


def gram_kernel(pieces, out):
    rows = pieces[0]
    for peer in range(1, pieces.shape[0]):
        rows = rows + pieces[peer]
    gram = lax.dot_general(
        rows, rows, (((1,), (1,)), ((), ())), preferred_element_type=jnp.float32, precision=lax.Precision.HIGHEST
    )
    gram = gram[:FIELDS, :FIELDS] + gram[FIELDS : 2 * FIELDS, FIELDS : 2 * FIELDS]
    wide = jnp.concatenate([gram, jnp.zeros((FIELDS, 128 - FIELDS), jnp.float32)], axis=1)
    line = wide[0:1]
    for f in range(1, FIELDS):
        line = line + pltpu.roll(wide[f : f + 1], PITCH * f, 1)
    out[...] = jnp.broadcast_to(line[None], out.shape)


def load_kernel(_, low, high, after, before, to_after, to_before, sem):
    ends = low.shape[0] - 6
    kept = to_after.shape[0] - 2 * ends
    copies = []
    for out, slab, start in ((to_after, after, 0), (to_before, before, kept)):
        for source, target in (
            (low.at[pl.ds(6, ends)], out.at[pl.ds(0, ends)]),
            (high.at[pl.ds(6, ends)], out.at[pl.ds(ends, ends)]),
            (slab.at[pl.ds(start, kept)], out.at[pl.ds(2 * ends, kept)]),
        ):
            copies.append(pltpu.make_async_copy(source, target, sem.at[len(copies)]))
    for copy in copies:
        copy.start()
    for copy in copies:
        copy.wait()


def wide_coefficients(kappa, mass, low, high):
    return jnp.concatenate([low[0], kappa, high[0]], axis=0), jnp.concatenate([low[1], mass, high[1]], axis=0) - 1.0


def fields_to(out, planes, places, s, wide_kappa, q, low_on, high_on):
    slab = wide_kappa.shape[0] - 6
    parts = []
    for (ref, first), size in zip(places, (3, slab, 3)):
        parts.append(planes[ref][pl.ds(first + s * size, size)])
    for f, field in enumerate(ten_fields(jnp.concatenate(parts, axis=0), wide_kappa, q, low_on, high_on)):
        out[f] = field.reshape(-1, field.shape[2])


def far_kernel(sections, edge, kappa, mass, low, high, halo_after, halo_before, after, before, out, *held):
    *held, sem = held
    here = out.shape[0]
    step = pl.program_id(0)
    copies = [pltpu.make_async_copy(*pair, sem.at[n]) for n, pair in enumerate(zip((after, before), held))]

    @pl.when(step == 0)
    def _():
        for copy in copies:
            copy.start()

    wide_kappa, q = wide_coefficients(kappa[...], mass[...], low, high)
    base = 0
    for (count, *places), copy in zip(sections, copies):

        @pl.when(step == base)
        def _(copy=copy):
            copy.wait()

        @pl.when((step >= base) & (step < base + count // here))
        def _(base=base, places=places):
            def one_source(i, carry):
                s = (step - base) * here + i
                planes = (halo_after, held[0], halo_before, held[1])
                fields_to(out.at[i], planes, places, s, wide_kappa, q, edge[0], edge[1])
                return carry

            lax.fori_loop(0, here, one_source, 0)

        base = base + count // here


def solve_small(gram):
    ridge = 0.001 * (gram[1][1] + gram[2][2] + gram[3][3]) / 3.0 + 1.0
    entry = [[gram[1 + i][1 + k] + (ridge if i == k else 0.0) for k in range(3)] for i in range(3)]
    h = [gram[1 + i][0] for i in range(3)]
    l00 = jnp.sqrt(entry[0][0])
    l10 = entry[1][0] / l00
    l20 = entry[2][0] / l00
    l11 = jnp.sqrt(entry[1][1] - l10 * l10)
    l21 = (entry[2][1] - l20 * l10) / l11
    l22 = jnp.sqrt(entry[2][2] - l20 * l20 - l21 * l21)
    f0 = h[0] / l00
    f1 = (h[1] - l10 * f0) / l11
    f2 = (h[2] - l20 * f0 - l21 * f1) / l22
    c2 = f2 / l22
    c1 = (f1 - l21 * c2) / l11
    c0 = (f0 - l10 * c1 - l20 * c2) / l00
    return c0, c1, c2


def relative_group(step, per):
    place = step // per
    return jnp.where(place == 2, 3, jnp.where(place == 3, 2, place))


def final_kernel(
    sections, group, table, ids, edge, kappa, mass, low, high, third_after, second_after, third_before, second_before,
    grams, near_hbm, beside_hbm, sol, res, near, far, turned, weights, scalars, sem, arrived,
):
    groups = 4
    per_group = grams.shape[0] // (groups * groups)
    shifts = ids.shape[0]
    step = pl.program_id(0)
    here = sol.shape[1]
    near_steps = per_group // here
    beside_steps = beside_hbm.shape[0] // here

    def fetch(n):
        if n == 0:
            return pltpu.make_async_copy(near_hbm, near, arrived.at[0])
        rows = pl.ds((n - 1) * here, here)
        return pltpu.make_async_copy(beside_hbm.at[rows], far.at[rows], arrived.at[n])

    copies = 1 + beside_steps

    @pl.when(step == 0)
    def _():
        for n in range(copies):
            fetch(n).start()
        parts = grams.shape[0] // (groups * per_group)
        flat = grams.reshape(grams.shape[0], 128)
        lines = []
        for g in range(groups):
            line = None
            for part in range(parts):
                one = flat[pl.ds(part * groups + g, per_group, stride=parts * groups), :]
                line = one if line is None else line + one
            lines.append(line)
        gram = jnp.concatenate(lines, axis=0)
        turned[...] = jnp.concatenate([gram, jnp.zeros((128 - gram.shape[0], 128), jnp.float32)], axis=0).T
        shape = (8, 128)
        line = lax.broadcasted_iota(jnp.int32, shape, 0)
        sigma = jnp.zeros(shape, jnp.float32)
        for j in range(shifts):
            sigma = jnp.where(line == j, table[ids[j]], sigma)
        terms = {}
        for f in range(FIELDS):
            for e in range(f, FIELDS):
                place = PITCH * f + e
                value = jnp.broadcast_to(turned[place : place + 1, :], shape)
                sign = SIGN[f] * SIGN[e] * (2.0 if LEVEL[f] == LEVEL[e] and f != e else 1.0)
                value = value if sign == 1.0 else value * sign
                key = (LEVEL[f], LEVEL[e], POWER[f] + POWER[e])
                terms[key] = terms[key] + value if key in terms else value
        inner = [[None] * 4 for _ in range(4)]
        for a in range(4):
            for b in range(a, 4):
                value = terms[(a, b, a + b)]
                for power in range(a + b - 1, -1, -1):
                    value = value * sigma + terms[(a, b, power)]
                value = value * (1.0 / 6.0 ** (a + b))
                inner[a][b] = inner[b][a] = value
        center = 6.0 + sigma
        mixed = [[6.0 * inner[i + 1][k] + center * inner[i][k] for k in range(4)] for i in range(3)]
        full = [[None] * 4 for _ in range(4)]
        for i in range(3):
            full[1 + i][0] = mixed[i][0]
            for k in range(3):
                full[1 + i][1 + k] = 6.0 * mixed[i][k + 1] + center * mixed[i][k]
        c0, c1, c2 = solve_small(full)
        values = (
            c0,
            c1 * (1.0 / 6.0),
            c2 * (1.0 / 36.0),
            1.0 - c0 * center,
            (6.0 * c0 + c1 * center) * (-1.0 / 6.0),
            (6.0 * c1 + c2 * center) * (-1.0 / 36.0),
            c2 * (-1.0 / 36.0),
        )
        for n, value in enumerate(values):
            weights[8 * n : 8 * (n + 1), :] = value
        copy = pltpu.make_async_copy(weights, scalars, sem)
        copy.start()
        wide_kappa, q = wide_coefficients(kappa[...], mass[...], low, high)
        planes = (third_after, second_after, third_before, second_before)
        base = beside_hbm.shape[0]
        for count, *places in sections:

            def one_source(s, carry, base=base, places=places):
                fields_to(far.at[base + s], planes, places, s, wide_kappa, q, edge[0], edge[1])
                return carry

            lax.fori_loop(0, count, one_source, 0)
            base = base + count
        copy.wait()

    ny = sol.shape[3]
    pitch = near.shape[0] // (FIELDS * per_group)
    steps_per_group = per_group // here
    ahead = relative_group(step, steps_per_group)
    first = lax.rem(group[0] + ahead, groups) * per_group + lax.rem(step, steps_per_group) * here

    def combine(read):
        for i in range(here):
            c = [[scalars[8 * n + j, first + i] for n in range(7)] for j in range(shifts)]
            for p in range(sol.shape[2]):
                w, e10, e01, e20, e11, e02, e30, e21, e12, e03 = (read(i, f, p * ny) for f in range(FIELDS))
                for j in range(shifts):
                    x = table[ids[j]]
                    c0, c1, c2, b0, b1, b2, b3 = c[j]
                    v1 = x * e01 - e10
                    v2 = x * (x * e02 - e11) + e20
                    v3 = x * (x * (x * e03 - e12) + e21) - e30
                    sol[j, i, p] = c0 * w + c1 * v1 + c2 * v2
                    res[j, i, p] = b0 * w + b1 * v1 + b2 * v2 + b3 * v3

    @pl.when(step < near_steps)
    def _():
        @pl.when(step == 0)
        def _():
            fetch(0).wait()

        def read(i, f, at):
            return near[pl.ds(pl.multiple_of((f * per_group + step * here + i) * pitch, 8) + at, ny), :]

        combine(read)

    @pl.when(step >= near_steps)
    def _():
        for n in range(1, copies):

            @pl.when(step == near_steps + n - 1)
            def _(n=n):
                fetch(n).wait()

        combine(lambda i, f, at: far[(step - near_steps) * here + i, f, at : at + ny, :])


def cost(us):
    return pl.CostEstimate(flops=int(us * 8e6), bytes_accessed=0, transcendentals=0)


def limit(mib):
    return pltpu.CompilerParams(vmem_limit_bytes=mib << 20)


def on_device(sources, kappa, mass, shift_table, shift_ids, sketch):
    f32 = jnp.float32
    dom, shift = lax.axis_size("dom"), lax.axis_size("shift")
    per_group, slab, ny, nz = sources.shape
    total = per_group * shift
    rows = sketch.shape[0]
    pairs = slab * ny // 2
    at = lax.axis_index("dom")
    edge = jnp.stack([at > 0, at < dom - 1]).astype(f32)
    group = lax.axis_index("shift").astype(jnp.int32)[None]

    HBM = pl.BlockSpec(memory_space=pltpu.HBM)

    def in_hbm(array):
        return pltpu.with_memory_space_constraint(array, pltpu.HBM)

    coeffs = (in_hbm(kappa), in_hbm(mass))
    ends = pltpu.VMEM((2 + per_group, 3, ny, nz), f32)
    top, bottom, own = pl.pallas_call(
        edges_kernel,
        in_specs=[HBM] * 3,
        out_specs=[VMEM] * 3,
        out_shape=[ends, ends, pltpu.VMEM((2 + per_group, slab, ny, nz), f32)],
        scratch_shapes=[pltpu.SemaphoreType.DMA((9,))],
        name="edges",
    )(*coeffs, in_hbm(sources))
    low = lax.ppermute(top, "dom", [(i, i + 1) for i in range(dom - 1)])
    high = lax.ppermute(bottom, "dom", [(i + 1, i) for i in range(dom - 1)])
    from_next = [(i, (i - 1) % shift) for i in range(shift)]
    from_last = [(i, (i + 1) % shift) for i in range(shift)]
    half = per_group // 2
    after = lax.ppermute(sources, "shift", from_next)
    before = lax.ppermute(sources, "shift", from_last)

    pitch = slab * ny + 8
    pieces, near = pl.pallas_call(
        sketch_kernel,
        in_specs=[SMEM] + [VMEM] * 3 + [HBM],
        out_specs=[VMEM, HBM],
        out_shape=[
            pltpu.VMEM((dom, 24, 128), f32),
            pltpu.HBM((FIELDS * per_group * pitch, nz), f32),
        ],
        scratch_shapes=[
            pltpu.VMEM((pairs, rows, 2, nz), jnp.bfloat16),
            pltpu.VMEM((FIELDS * per_group * pitch, nz), f32),
            pltpu.VMEM((256, pairs * nz), jnp.bfloat16),
            pltpu.VMEM((2 * rows, 128), f32),
            pltpu.VMEM((2 * rows, 128), f32),
            pltpu.VMEM((rows // 128, 128, 128), f32),
            pltpu.SemaphoreType.DMA((CHUNKS,)),
            pltpu.SemaphoreType.DMA,
        ],
        compiler_params=limit(36),
        cost_estimate=cost(12),
        name="sketch_fields",
    )(edge, low, high, own, in_hbm(sketch.reshape(rows, pairs, 2, nz)))
    arrived = lax.all_to_all(pieces, "dom", 0, 0, tiled=True)

    def flat(array):
        return array.reshape(-1, ny, nz)

    ends, skip = 3 * per_group, 3 * half
    load = pltpu.VMEM((2 * ends + half * slab, ny, nz), f32)
    load_after, load_before = pl.pallas_call(
        load_kernel,
        in_specs=[HBM] + [pl.BlockSpec(memory_space=pl.ANY)] * 2 + [HBM] * 2,
        out_specs=[VMEM] * 2,
        out_shape=[load, load],
        scratch_shapes=[pltpu.SemaphoreType.DMA((6,))],
        name="load",
    )(near, flat(low), flat(high), in_hbm(flat(after)), in_hbm(flat(before)))
    second_after = lax.ppermute(load_after, "shift", from_next)
    second_before = lax.ppermute(load_before, "shift", from_last)

    def third(array, start):
        return jnp.concatenate([array[start : start + skip], array[ends + start : ends + start + skip]])

    third_after = lax.ppermute(third(second_after, 0), "shift", from_next)
    third_before = lax.ppermute(third(second_before, skip), "shift", from_last)

    lines = pl.pallas_call(
        gram_kernel,
        in_specs=[VMEM],
        out_specs=VMEM,
        out_shape=pltpu.VMEM((dom * shift, 1, 128), f32),
        cost_estimate=cost(2),
        name="gram",
    )(pltpu.with_memory_space_constraint(arrived, pltpu.VMEM))
    grams = lax.all_to_all(lines, BOTH, 0, 0, tiled=True)
    far_here = 4
    far_shape = (2 * per_group, FIELDS, slab * ny, nz)
    slabs = pltpu.VMEM((per_group * slab, ny, nz), f32)
    beside = pl.pallas_call(
        functools.partial(
            far_kernel,
            ((per_group, (0, 0), (1, 0), (0, ends)), (per_group, (2, 0), (3, 0), (2, ends))),
        ),
        in_specs=[SMEM] + [VMEM] * 6 + [HBM] * 2,
        grid=(far_shape[0] // far_here,),
        out_specs=pl.BlockSpec((far_here, *far_shape[1:]), lambda i: (i, 0, 0, 0)),
        out_shape=pltpu.HBM(far_shape, f32),
        scratch_shapes=[slabs, slabs, pltpu.SemaphoreType.DMA((2,))],
        compiler_params=limit(20),
        cost_estimate=cost(6),
        name="fields_beside",
    )(edge, kappa, mass, low, high, second_after, second_before, in_hbm(flat(after)), in_hbm(flat(before)))
    sections = (
        (half, (0, 0), (1, 2 * ends), (0, skip)),
        (half, (2, 0), (3, 2 * ends), (2, skip)),
    )

    here = per_group
    steps = total // here
    shifts = shift_ids.shape[0]
    per = per_group // here

    def place(i, group):
        return (0, lax.rem(group[0] + relative_group(i, per), shift) * per + lax.rem(i, per), 0, 0, 0)

    spec = pl.BlockSpec((shifts, here, slab, ny, nz), place)
    shape = jax.ShapeDtypeStruct((shifts, total, slab, ny, nz), f32)
    return pl.pallas_call(
        functools.partial(final_kernel, sections),
        grid_spec=pltpu.PrefetchScalarGridSpec(
            num_scalar_prefetch=1,
            grid=(steps,),
            in_specs=[SMEM] * 3 + [VMEM] * 9 + [HBM] * 2,
            out_specs=[spec, spec],
            scratch_shapes=[
                pltpu.VMEM(near.shape, f32),
                pltpu.VMEM((total - per_group, FIELDS, slab * ny, nz), f32),
                pltpu.VMEM((128, 128), f32),
                pltpu.VMEM((56, 128), f32),
                pltpu.SMEM((56, 128), f32),
                pltpu.SemaphoreType.DMA,
                pltpu.SemaphoreType.DMA((1 + far_shape[0] // here,)),
            ],
        ),
        out_shape=[shape, shape],
        compiler_params=limit(36),
        name="combine",
    )(
        group, shift_table, shift_ids, edge, kappa, mass, low, high,
        third_after, second_after, third_before, second_before,
        grams, in_hbm(near), in_hbm(beside),
    )


def solution(mesh):
    placed = (
        P("shift", "dom", None, None),
        P("dom", None, None),
        P("dom", None, None),
        P(),
        P("shift"),
        P(None, "dom", None, None),
    )

    def body(*args):
        return tuple(on_device(*args))

    return jax.shard_map(
        body,
        mesh=mesh,
        in_specs=placed,
        out_specs=(P("shift", None, "dom", None, None), P("shift", None, "dom", None, None)),
        check_vma=False,
    )
```
